8 devices in a mesh: data: 2 (over z, y), cp: 4 (over x, core).
Axes of the slice: x: 2, y: 2, z: 1, core: 2. Of those that a mesh axis runs over, the one named last changes fastest.
Arguments:
- q: bfloat16 [64, 1024, 12, 128], P('data', 'cp'), parts along dimension 0
- k: bfloat16 [64, 1024, 2, 128], P('data', 'cp'), parts along dimension 0
- v: bfloat16 [64, 1024, 2, 128], P('data', 'cp'), parts along dimension 0
- do: bfloat16 [64, 1024, 12, 128], P('data', 'cp'), parts along dimension 0
- o: bfloat16 [64, 1024, 12, 128], P('data', 'cp'), parts along dimension 0
- lse: float32 [64, 12, 1024], P('data', None, 'cp'), parts along dimension 0
Outputs:
- output 1: bfloat16 [64, 1024, 12, 128], P('data', 'cp'), parts along dimension 0
- output 2: bfloat16 [64, 1024, 2, 128], P('data', 'cp'), parts along dimension 0
- output 3: bfloat16 [64, 1024, 2, 128], P('data', 'cp'), parts along dimension 0
There are 2 independent parts. The reference program is written for one: setup_inputs(seed, part) draws one part's arguments, and reference() takes and returns one part's arrays. A program takes and returns all parts, laid end to end along the dimension named above; each array names one.
All inputs are finite; a program needn't handle non-finite values.
Results may differ from the reference program's by a relative error of at most 0.001.
Values are sent between devices in bfloat16 or wider.
A program may use at most 1 GiB of HBM per device.

```python
import math
import numpy as np
import jax
import jax.numpy as jnp
from jax import lax

CP = 4
TDEV = 256
B = 32
HQ = 12
HKV = 2
HEAD = 128

C = TDEV // 2
NCH = 2 * CP
S = CP * TDEV
G = HQ // HKV
SCALE = HEAD ** -0.5
DO_STD = (S / math.log(S)) ** 0.5
ORDER = np.array([c for r in range(CP) for c in (r, NCH - 1 - r)])
INVERSE = np.argsort(ORDER)


def _reorder(x, axis, perm):
    xs = x.reshape(x.shape[:axis] + (NCH, C) + x.shape[axis + 1:])
    return jnp.take(xs, perm, axis=axis).reshape(x.shape)


def _forward(q, k, v):
    f = jnp.float32
    qc = q.reshape(B, NCH, C, HKV, G, HEAD).transpose(1, 0, 2, 3, 4, 5)
    kc = k.reshape(B, NCH, C, HKV, HEAD).transpose(1, 0, 2, 3, 4)
    vc = v.reshape(B, NCH, C, HKV, HEAD).transpose(1, 0, 2, 3, 4)
    idx = jnp.arange(C)

    def per_query(xs):
        qa, a = xs
        qf = qa.astype(f)

        def body(carry, ys):
            m, l, acc = carry
            kb, vb, b = ys
            s = jnp.einsum('bqhgd,bkhd->bhgqk', qf, kb.astype(f)) * SCALE
            mask = (a * C + idx)[:, None] >= (b * C + idx)[None, :]
            s = jnp.where(mask, s, -jnp.inf)
            m_new = jnp.maximum(m, jnp.max(s, axis=-1))
            p = jnp.exp(s - m_new[..., None])
            corr = jnp.exp(m - m_new)
            l = l * corr + jnp.sum(p, axis=-1)
            acc = acc * corr[..., None] + jnp.einsum('bhgqk,bkhd->bhgqd', p, vb.astype(f))
            return (m_new, l, acc), None

        init = (jnp.full((B, HKV, G, C), -jnp.inf, f), jnp.zeros((B, HKV, G, C), f),
                jnp.zeros((B, HKV, G, C, HEAD), f))
        (m, l, acc), _ = lax.scan(body, init, (kc, vc, jnp.arange(NCH)))
        return acc / l[..., None], m + jnp.log(l)

    o, lse = lax.map(per_query, (qc, jnp.arange(NCH)))
    o = o.transpose(1, 0, 4, 2, 3, 5).reshape(B, S, HQ, HEAD).astype(jnp.bfloat16)
    lse = lse.transpose(1, 2, 3, 0, 4).reshape(B, HQ, S)
    return o, lse


def setup_inputs(seed: int = 0, part: int = 0) -> dict:
    key = jax.random.fold_in(jax.random.PRNGKey(seed), part)
    kq, kk, kv, kd = jax.random.split(key, 4)
    q = jax.random.normal(kq, (B, S, HQ, HEAD), jnp.float32).astype(jnp.bfloat16)
    k = jax.random.normal(kk, (B, S, HKV, HEAD), jnp.float32).astype(jnp.bfloat16)
    v = jax.random.normal(kv, (B, S, HKV, HEAD), jnp.float32).astype(jnp.bfloat16)
    do = (jax.random.normal(kd, (B, S, HQ, HEAD), jnp.float32) * DO_STD).astype(jnp.bfloat16)
    o, lse = _forward(q, k, v)
    return {'q': _reorder(q, 1, ORDER), 'k': _reorder(k, 1, ORDER), 'v': _reorder(v, 1, ORDER),
            'do': do, 'o': _reorder(o, 1, ORDER), 'lse': _reorder(lse, 2, ORDER)}


def _pair(qa, doa, la, da, kb, vb, a, b):
    f = jnp.float32
    idx = jnp.arange(C)
    s = jnp.einsum('bqhgd,bkhd->bhgqk', qa.astype(f), kb.astype(f)) * SCALE
    mask = (a * C + idx)[:, None] >= (b * C + idx)[None, :]
    p = jnp.exp(jnp.where(mask, s - la[..., None], -jnp.inf))
    pb = p.astype(jnp.bfloat16).astype(f)
    dv = jnp.einsum('bhgqk,bqhgd->bkhd', pb, doa.astype(f))
    dp = jnp.einsum('bqhgd,bkhd->bhgqk', doa.astype(f), vb.astype(f))
    ds = (p * (dp - da[..., None])).astype(jnp.bfloat16).astype(f)
    dq = jnp.einsum('bhgqk,bkhd->bqhgd', ds, kb.astype(f))
    dk = jnp.einsum('bhgqk,bqhgd->bkhd', ds, qa.astype(f))
    return dq, dk, dv


def reference(q, k, v, do, o, lse):
    f = jnp.float32
    q, k, v, do, o = (_reorder(x, 1, INVERSE) for x in (q, k, v, do, o))
    lse = _reorder(lse, 2, INVERSE)
    delta = jnp.sum(do.astype(f) * o.astype(f), axis=-1).transpose(0, 2, 1)
    qc = q.reshape(B, NCH, C, HKV, G, HEAD).transpose(1, 0, 2, 3, 4, 5)
    doc = do.reshape(B, NCH, C, HKV, G, HEAD).transpose(1, 0, 2, 3, 4, 5)
    kc = k.reshape(B, NCH, C, HKV, HEAD).transpose(1, 0, 2, 3, 4)
    vc = v.reshape(B, NCH, C, HKV, HEAD).transpose(1, 0, 2, 3, 4)
    lc = lse.reshape(B, HKV, G, NCH, C).transpose(3, 0, 1, 2, 4)
    dc = delta.reshape(B, HKV, G, NCH, C).transpose(3, 0, 1, 2, 4)

    def outer(carry, xs):
        dk_acc, dv_acc = carry
        qa, doa, la, da, a = xs

        def inner(dq, ys):
            kb, vb, b = ys
            dq_c, dk_c, dv_c = _pair(qa, doa, la, da, kb, vb, a, b)
            return dq + dq_c, (dk_c, dv_c)

        dq, (dkc, dvc) = lax.scan(inner, jnp.zeros((B, C, HKV, G, HEAD), f), (kc, vc, jnp.arange(NCH)))
        return (dk_acc + dkc, dv_acc + dvc), dq

    zeros = jnp.zeros((NCH, B, C, HKV, HEAD), f)
    (dk, dv), dq = lax.scan(outer, (zeros, zeros), (qc, doc, lc, dc, jnp.arange(NCH)))
    dq = (dq * SCALE).transpose(1, 0, 2, 3, 4, 5).reshape(B, S, HQ, HEAD).astype(jnp.bfloat16)
    dk = (dk * SCALE).transpose(1, 0, 2, 3, 4).reshape(B, S, HKV, HEAD).astype(jnp.bfloat16)
    dv = dv.transpose(1, 0, 2, 3, 4).reshape(B, S, HKV, HEAD).astype(jnp.bfloat16)
    return (_reorder(dq, 1, ORDER), _reorder(dk, 1, ORDER), _reorder(dv, 1, ORDER))
```

```python
import functools
import jax
import jax.numpy as jnp
from jax import lax
from jax.experimental import pallas as pl
from jax.experimental.pallas import tpu as pltpu
from jax.sharding import PartitionSpec as P

F32 = jnp.float32
BF16 = jnp.bfloat16
MESH = pl.DeviceIdType.MESH

C = 128
GB = 4
NP = 4
LAG = 7
NO = 8

OWN, PARTNER, PEER, DIAG = 0, 1, 2, 3


def _dot(a, b):
    return lax.dot_general(a, b, (((1,), (0,)), ((), ())), preferred_element_type=F32)


def _kernel(nb, hkv, grp, scale,
            q_ref, do_ref, o_ref, lse_ref, k_hbm, v_hbm,
            dq_ref, dk_ref, dv_ref, rl_hbm,
            kl, vl, acc, dl, ps, osum, buf, qt, dot_, dqt, lse_s, del_s,
            loc_sem, xs_sem, xr_sem, es_sem, er_sem, fs_sem, fr_sem,
            ds_sem, dr_sem, ps_sem, pr_sem, buf_sem, credit):
    i = pl.program_id(0)
    r = lax.axis_index('cp')
    chip = r // 2
    odd = lax.rem(r, 2)
    peer = r + 1 - 2 * odd
    partner = lax.rem(r + 2, 4)
    ng = nb // GB
    rows = grp * C

    def kv(which):
        return (k_hbm, kl) if which == 0 else (v_hbm, vl)

    def local_copy(j, w):
        src, dst = kv(w)
        b = pl.ds(j * GB, GB)
        return pltpu.make_async_copy(src.at[b], dst.at[b, OWN], loc_sem.at[j, w])

    def peer_copy(j, w):
        src, dst = kv(w)
        b = pl.ds(j * GB, GB)
        return pltpu.make_async_remote_copy(src.at[b], dst.at[b, PEER], es_sem.at[j, w], er_sem.at[j, w],
                                            device_id={'cp': peer}, device_id_type=MESH)

    def x_copy(j, w, full):
        src, dst = kv(w)
        b = pl.ds(j * GB, GB)
        t = pl.ds(0, 2 * C if full else C)
        return pltpu.make_async_remote_copy(src.at[b, :, t], dst.at[b, PARTNER, :, t], xs_sem.at[j, w], xr_sem.at[j, w],
                                            device_id={'cp': partner}, device_id_type=MESH)

    def fwd_copy(j, w, full):
        _, dst = kv(w)
        b = pl.ds(j * GB, GB)
        t = pl.ds(0, 2 * C if full else C)
        return pltpu.make_async_remote_copy(dst.at[b, PARTNER, :, t], dst.at[b, DIAG, :, t], fs_sem.at[j, w], fr_sem.at[j, w],
                                            device_id={'cp': peer}, device_id_type=MESH)

    def part_copy(m):
        s = lax.rem(m, 2)
        return pltpu.make_async_remote_copy(acc.at[s, pl.ds(4, 4)], dl.at[s], ds_sem.at[s], dr_sem.at[s],
                                            device_id={'cp': peer}, device_id_type=MESH)

    def sum_copy(m, full):
        s = lax.rem(m, NP)
        n = pl.ds(0, 2 if full else 1)
        return pltpu.make_async_remote_copy(ps.at[s, n], rl_hbm.at[m, n], ps_sem.at[s], pr_sem.at[m],
                                            device_id={'cp': partner}, device_id_type=MESH)

    def forward(j):
        for c, full in ((0, True), (1, False)):
            @pl.when(chip == c)
            def _():
                for w in range(2):
                    x_copy(j, w, full).wait_recv()
                    fwd_copy(j, w, full).start()

    @pl.when(i == 0)
    def _():
        barrier = pltpu.get_barrier_semaphore()
        for other in (peer, partner):
            pl.semaphore_signal(barrier, inc=1, device_id={'cp': other}, device_id_type=MESH)
        pl.semaphore_wait(barrier, 2)

        @pl.loop(0, ng)
        def _(j):
            for c, full in ((0, False), (1, True)):
                @pl.when(chip == c)
                def _():
                    for w in range(2):
                        x_copy(j, w, full).start()
            for w in range(2):
                local_copy(j, w).start()
                peer_copy(j, w).start()
        buf[...] = jnp.zeros_like(buf)
        forward(0)

    @pl.when(i < nb)
    def _():
        b = i
        slot = lax.rem(i, 2)
        j = i // GB

        @pl.when(lax.rem(i, GB) == 0)
        def _():
            for w in range(2):
                local_copy(j, w).wait()
                peer_copy(j, w).wait_recv()
            for c, full in ((0, True), (1, False)):
                @pl.when(chip == c)
                def _():
                    for w in range(2):
                        fwd_copy(j, w, full).wait_recv()

        @pl.when((lax.rem(i, GB) == GB // 2) & (i < nb - GB))
        def _():
            forward(j + 1)

        acc[slot] = jnp.zeros(acc.shape[1:], F32)
        dqt[...] = jnp.zeros_like(dqt)
        row = lax.rem(i, 8)
        for g in range(hkv):
            for hh in range(grp):
                h = g * grp + hh
                lanes = pl.ds(hh * C, C)
                lse_row = lse_ref[h, pl.ds(row, 1), :]
                for sg in range(2):
                    tok = pl.ds(sg * C, C)
                    dob = do_ref[0, h, tok, :]
                    qt[sg, g, :, lanes] = q_ref[0, h, tok, :].T
                    dot_[sg, g, :, lanes] = dob.T
                    prod = dob.astype(F32) * o_ref[0, h, tok, :].astype(F32)
                    del_s[sg, g, :, lanes] = jnp.sum(prod.T, axis=0, keepdims=True)
                    lse_s[sg, g, :, lanes] = lse_row[:, sg * C:(sg + 1) * C]

        def pair(qs, ks, shift):
            sec, half = ks // 2, lax.rem(ks, 2)
            keys = pl.ds(pl.multiple_of(half * C, C), C)
            toks = pl.ds(pl.multiple_of(qs * C, C), C)
            for g in range(hkv):
                k = kl[b, sec, g, keys, :]
                v = vl[b, sec, g, keys, :]
                heads = pl.ds(g * grp, grp)
                s = _dot(k, qt[qs, g])
                p = jnp.exp(s * scale - lse_s[qs, g])
                if shift is not None:
                    ki = lax.broadcasted_iota(jnp.int32, (C, rows), 0)
                    qi = lax.bitwise_and(lax.broadcasted_iota(jnp.int32, (C, rows), 1), C - 1)
                    p = jnp.where(ki <= qi + shift, p, 0.0)
                dp = _dot(v, dot_[qs, g])
                ds = (p * (dp - del_s[qs, g])).astype(BF16)
                acc[slot, ks, g, 1] += _dot(p.astype(BF16), do_ref[0, heads, toks, :].reshape(rows, C))
                acc[slot, ks, g, 0] += _dot(ds, q_ref[0, heads, toks, :].reshape(rows, C))
                dqt[qs, g] += _dot(k.T, ds)

        @pl.loop(0, 3)
        def _(t):
            pair((t + 1) // 2, t // 2, C * lax.rem(t, 2))

        @pl.loop(0, 2)
        def _(t):
            pair(1 - odd * (1 - t), 4 + t * (1 - odd), None)

        @pl.loop(0, 4)
        def _(t):
            u = (1 - chip) * t + chip * 2 * (t // 2)
            pair((1 - chip) + chip * lax.rem(t, 2), 2 + lax.rem(u, 2) + 4 * (u // 2), None)

        for g in range(hkv):
            for hh in range(grp):
                for sg in range(2):
                    x = dqt[sg, g, :, pl.ds(hh * C, C)].T
                    dq_ref[0, g * grp + hh, pl.ds(sg * C, C), :] = (x * scale).astype(BF16)

        @pl.when(i >= 2)
        def _():
            pl.semaphore_wait(credit, 1)
        part_copy(i).start()

    @pl.when((i >= 1) & (i <= nb))
    def _():
        m = i - 1
        s = lax.rem(m, 2)
        s4 = lax.rem(m, NP)
        copy = part_copy(m)
        copy.wait_send()
        copy.wait_recv()
        osum[lax.rem(m, NO)] = acc[s, pl.ds(0, 2)] + dl[s, pl.ds(0, 2)]
        for c, full in ((0, True), (1, False)):
            @pl.when((chip == c) & (m >= NP))
            def _():
                sum_copy(m - NP, full).wait_send()
        ps[s4] = acc[s, pl.ds(2, 2)] + dl[s, pl.ds(2, 2)]

        @pl.when(m < nb - 2)
        def _():
            pl.semaphore_signal(credit, inc=1, device_id={'cp': peer}, device_id_type=MESH)
        for c, full in ((0, True), (1, False)):
            @pl.when(chip == c)
            def _():
                sum_copy(m, full).start()

    @pl.when(i >= LAG)
    def _():
        m = i - LAG
        for c, full in ((0, False), (1, True)):
            @pl.when(chip == c)
            def _():
                sum_copy(m, full).wait_recv()
                n = pl.ds(0, 2 if full else 1)
                copy = pltpu.make_async_copy(rl_hbm.at[m, n], buf.at[n], buf_sem)
                copy.start()
                copy.wait()
        so = lax.rem(m, NO)
        for sg in range(2):
            for g in range(hkv):
                tok = pl.ds(sg * C, C)
                dk_ref[0, g, tok, :] = ((osum[so, sg, g, 0] + buf[sg, g, 0]) * scale).astype(BF16)
                dv_ref[0, g, tok, :] = (osum[so, sg, g, 1] + buf[sg, g, 1]).astype(BF16)

    @pl.when(i == nb + LAG - 1)
    def _():
        for c, full in ((0, True), (1, False)):
            @pl.when(chip == c)
            def _():
                for m in range(nb - NP, nb):
                    sum_copy(m, full).wait_send()

        @pl.loop(0, ng)
        def _(j):
            for w in range(2):
                peer_copy(j, w).wait_send()
            for c, full in ((0, False), (1, True)):
                @pl.when(chip == c)
                def _():
                    for w in range(2):
                        x_copy(j, w, full).wait_send()
                        fwd_copy(j, w, not full).wait_send()


def solution(mesh):
    def local(q, k, v, do, o, lse):
        b, t, hq, d = q.shape
        hkv = k.shape[2]
        grp = hq // hkv
        scale = d ** -0.5
        ng = b // GB
        heads = lambda x: jnp.transpose(x, (0, 2, 1, 3))
        q, do, o, k, v = (heads(x) for x in (q, do, o, k, v))
        lse = jnp.transpose(lse, (1, 0, 2))

        last = b - 1
        big = pl.BlockSpec((1, hq, t, d), lambda i: (jnp.minimum(i, last), 0, 0, 0))
        out = pl.BlockSpec((1, hkv, t, d), lambda i: (jnp.maximum(i - LAG, 0), 0, 0, 0))
        anyspec = pl.BlockSpec(memory_space=pl.ANY)
        dma = pltpu.SemaphoreType.DMA
        flops = 9 * b * hq * 5 * 2 * C * C * d
        dq, dk, dv, _ = pl.pallas_call(
            functools.partial(_kernel, b, hkv, grp, scale),
            grid=(b + LAG,),
            in_specs=[big, big, big,
                      pl.BlockSpec((hq, 8, t), lambda i: (0, jnp.minimum(i, last) // 8, 0)),
                      anyspec, anyspec],
            out_specs=[big, out, out, anyspec],
            out_shape=[jax.ShapeDtypeStruct((b, hq, t, d), BF16),
                       jax.ShapeDtypeStruct((b, hkv, t, d), BF16),
                       jax.ShapeDtypeStruct((b, hkv, t, d), BF16),
                       jax.ShapeDtypeStruct((b, 2, hkv, 2, C, d), F32)],
            scratch_shapes=[
                pltpu.VMEM((b, 4, hkv, t, d), BF16),
                pltpu.VMEM((b, 4, hkv, t, d), BF16),
                pltpu.VMEM((2, 8, hkv, 2, C, d), F32),
                pltpu.VMEM((2, 4, hkv, 2, C, d), F32),
                pltpu.VMEM((NP, 2, hkv, 2, C, d), F32),
                pltpu.VMEM((NO, 2, hkv, 2, C, d), F32),
                pltpu.VMEM((2, hkv, 2, C, d), F32),
                pltpu.VMEM((2, hkv, d, grp * C), BF16),
                pltpu.VMEM((2, hkv, d, grp * C), BF16),
                pltpu.VMEM((2, hkv, d, grp * C), F32),
                pltpu.VMEM((2, hkv, 1, grp * C), F32),
                pltpu.VMEM((2, hkv, 1, grp * C), F32),
                dma((ng, 2)), dma((ng, 2)), dma((ng, 2)), dma((ng, 2)), dma((ng, 2)), dma((ng, 2)), dma((ng, 2)),
                dma((2,)), dma((2,)), dma((NP,)), dma((b,)), dma(()), pltpu.SemaphoreType.REGULAR,
            ],
            compiler_params=pltpu.CompilerParams(
                dimension_semantics=('arbitrary',), collective_id=0, has_side_effects=True,
                vmem_limit_bytes=67043328),
            cost_estimate=pl.CostEstimate(flops=flops, bytes_accessed=4 * q.size * 2, transcendentals=0),
        )(q, do, o, lse, k, v)
        return heads(dq), heads(dk), heads(dv)

    spec = P('data', 'cp')
    return jax.shard_map(local, mesh=mesh, in_specs=(spec, spec, spec, spec, spec, P('data', None, 'cp')),
                         out_specs=(spec, spec, spec), check_vma=False)
```

```python
import functools
import jax
import jax.numpy as jnp
from jax import lax
from jax.experimental import pallas as pl
from jax.experimental.pallas import tpu as pltpu
from jax.sharding import PartitionSpec as P

F32 = jnp.float32
BF16 = jnp.bfloat16
MESH = pl.DeviceIdType.MESH

C = 128
GB = 4
NP = 4
LAG = 7
NO = 8
AHEAD = 3
RS, R0 = 6, 2
RLAG = 6

OWN, PARTNER, PEER, DIAG = 0, 1, 2, 3


def _dot(a, b):
    return lax.dot_general(a, b, (((1,), (0,)), ((), ())), preferred_element_type=F32)


def _kernel(nb, hkv, grp, scale,
            q_ref, do_ref, o_ref, lse_ref, k_hbm, v_hbm,
            dq_ref, dk_hbm, dv_hbm, rl_hbm,
            kl, vl, kd, acc, dl, ps, osum, buf, ret, rps, fin, stage, qt, dot_, dqt, lse_s, del_s,
            loc_sem, xs_sem, xr_sem, es_sem, er_sem, fs_sem, fr_sem,
            ds_sem, dr_sem, ps_sem, pr_sem, buf_sem, os_sem, rs_sem, rr_sem, ts_sem, tr_sem, credit):
    i = pl.program_id(0)
    r = lax.axis_index('cp')
    chip = r // 2
    odd = lax.rem(r, 2)
    peer = r + 1 - 2 * odd
    partner = lax.rem(r + 2, 4)
    ng = nb // GB
    rows = grp * C

    def kv(which):
        return (k_hbm, kl) if which == 0 else (v_hbm, vl)

    def local_copy(j, w):
        src, dst = kv(w)
        b = pl.ds(j * GB, GB)
        return pltpu.make_async_copy(src.at[b], dst.at[b, OWN], loc_sem.at[j, w])

    def peer_copy(j, w):
        src, dst = kv(w)
        b = pl.ds(j * GB, GB)
        return pltpu.make_async_remote_copy(src.at[b], dst.at[b, PEER], es_sem.at[j, w], er_sem.at[j, w],
                                            device_id={'cp': peer}, device_id_type=MESH)

    def x_copy(j, w, full):
        src, dst = kv(w)
        b = pl.ds(j * GB, GB)
        t = pl.ds(0, 2 * C if full else C)
        return pltpu.make_async_remote_copy(src.at[b, t], dst.at[b, PARTNER, t], xs_sem.at[j, w], xr_sem.at[j, w],
                                            device_id={'cp': partner}, device_id_type=MESH)

    def fwd_copy(j, w, full):
        _, dst = kv(w)
        b = pl.ds(j * GB, GB)
        t = pl.ds(0, 2 * C if full else C)
        return pltpu.make_async_remote_copy(dst.at[b, PARTNER, t], dst.at[b, DIAG, t], fs_sem.at[j, w], fr_sem.at[j, w],
                                            device_id={'cp': peer}, device_id_type=MESH)

    def part_copy(m):
        s = lax.rem(m, 2)
        return pltpu.make_async_remote_copy(acc.at[s, pl.ds(4, 4)], dl.at[s], ds_sem.at[s], dr_sem.at[s],
                                            device_id={'cp': peer}, device_id_type=MESH)

    def sum_copy(m, full):
        s = lax.rem(m, NP)
        n = pl.ds(0, 2 if full else 1)
        return pltpu.make_async_remote_copy(ps.at[s, n], rl_hbm.at[m, n], ps_sem.at[s], pr_sem.at[m],
                                            device_id={'cp': partner}, device_id_type=MESH)

    def ret_copy(m):
        n = m // RS
        return pltpu.make_async_remote_copy(osum.at[lax.rem(m, NO)], ret.at[n], rs_sem.at[lax.rem(n, 2)], rr_sem.at[n],
                                            device_id={'cp': partner}, device_id_type=MESH)

    def fin_copy(m, w):
        dst = (dk_hbm, dv_hbm)[w]
        return pltpu.make_async_remote_copy(fin.at[w], dst.at[m], ts_sem.at[w], tr_sem.at[m // RS, w],
                                            device_id={'cp': partner}, device_id_type=MESH)

    def out_copy(m, w):
        dst = (dk_hbm, dv_hbm)[w]
        return pltpu.make_async_copy(stage.at[w], dst.at[m], os_sem.at[w])

    def results(dst, a, a_slot, b_, b_slot):
        for sg in range(2):
            for w in range(2):
                x = [a[(*a_slot, sg, g, w)] + b_[(*b_slot, sg, g, w)] for g in range(hkv)]
                if w == 0:
                    x = [y * scale for y in x]
                dst[w, pl.ds(sg * C, C)] = jnp.stack(x, axis=1).astype(BF16)

    def forward(j):
        for c, full in ((0, True), (1, False)):
            @pl.when(chip == c)
            def _():
                for w in range(2):
                    x_copy(j, w, full).wait_recv()
                    fwd_copy(j, w, full).start()

    @pl.when(i == 0)
    def _():
        barrier = pltpu.get_barrier_semaphore()
        for other in (peer, partner):
            pl.semaphore_signal(barrier, inc=1, device_id={'cp': other}, device_id_type=MESH)
        pl.semaphore_wait(barrier, 2)

        @pl.loop(0, ng)
        def _(j):
            for c, full in ((0, False), (1, True)):
                @pl.when((chip == c) if c == 0 else ((chip == c) & (j < AHEAD)))
                def _():
                    for w in range(2):
                        x_copy(j, w, full).start()
            for w in range(2):
                local_copy(j, w).start()
                peer_copy(j, w).start()
        buf[...] = jnp.zeros_like(buf)
        forward(0)

    @pl.when(i < nb)
    def _():
        b = i
        slot = lax.rem(i, 2)
        j = i // GB

        @pl.when(lax.rem(i, GB) == 0)
        def _():
            for w in range(2):
                local_copy(j, w).wait()
                peer_copy(j, w).wait_recv()
            for c, full in ((0, True), (1, False)):
                @pl.when(chip == c)
                def _():
                    for w in range(2):
                        fwd_copy(j, w, full).wait_recv()

        @pl.when((lax.rem(i, GB) == 0) & (chip == 1) & (j >= 1) & (j < ng - AHEAD + 1))
        def _():
            for w in range(2):
                x_copy(j + AHEAD - 1, w, True).start()

        @pl.when((lax.rem(i, GB) == GB // 2) & (i < nb - GB))
        def _():
            forward(j + 1)

        acc[slot] = jnp.zeros(acc.shape[1:], F32)
        dqt[...] = jnp.zeros_like(dqt)
        row = lax.rem(i, 8)
        for w in range(2):
            for sec in range(4):
                kd[w, sec] = jnp.transpose(kv(w)[1][b, sec], (1, 0, 2))
        for g in range(hkv):
            for hh in range(grp):
                h = g * grp + hh
                lanes = pl.ds(hh * C, C)
                lse_row = lse_ref[h, pl.ds(row, 1), :]
                for sg in range(2):
                    tok = pl.ds(sg * C, C)
                    dob = do_ref[0, h, tok, :]
                    qt[sg, g, :, lanes] = q_ref[0, h, tok, :].T
                    dot_[sg, g, :, lanes] = dob.T
                    prod = dob.astype(F32) * o_ref[0, h, tok, :].astype(F32)
                    del_s[sg, g, :, lanes] = jnp.sum(prod.T, axis=0, keepdims=True)
                    lse_s[sg, g, :, lanes] = lse_row[:, sg * C:(sg + 1) * C]

        def pair(qs, ks, shift):
            sec, half = ks // 2, lax.rem(ks, 2)
            keys = pl.ds(pl.multiple_of(half * C, C), C)
            toks = pl.ds(pl.multiple_of(qs * C, C), C)
            for g in range(hkv):
                k = kd[0, sec, g, keys, :]
                v = kd[1, sec, g, keys, :]
                heads = pl.ds(g * grp, grp)
                s = _dot(k, qt[qs, g])
                p = jnp.exp(s * scale - lse_s[qs, g])
                if shift is not None:
                    ki = lax.broadcasted_iota(jnp.int32, (C, rows), 0)
                    qi = lax.bitwise_and(lax.broadcasted_iota(jnp.int32, (C, rows), 1), C - 1)
                    p = jnp.where(ki <= qi + shift, p, 0.0)
                dp = _dot(v, dot_[qs, g])
                ds = (p * (dp - del_s[qs, g])).astype(BF16)
                acc[slot, ks, g, 1] += _dot(p.astype(BF16), do_ref[0, heads, toks, :].reshape(rows, C))
                acc[slot, ks, g, 0] += _dot(ds, q_ref[0, heads, toks, :].reshape(rows, C))
                dqt[qs, g] += _dot(k.T, ds)

        @pl.loop(0, 3)
        def _(t):
            pair((t + 1) // 2, t // 2, C * lax.rem(t, 2))

        @pl.loop(0, 2)
        def _(t):
            pair(1 - odd * (1 - t), 4 + t * (1 - odd), None)

        @pl.loop(0, 4)
        def _(t):
            u = (1 - chip) * t + chip * 2 * (t // 2)
            pair((1 - chip) + chip * lax.rem(t, 2), 2 + lax.rem(u, 2) + 4 * (u // 2), None)

        for g in range(hkv):
            for hh in range(grp):
                for sg in range(2):
                    x = dqt[sg, g, :, pl.ds(hh * C, C)].T
                    dq_ref[0, g * grp + hh, pl.ds(sg * C, C), :] = (x * scale).astype(BF16)

        @pl.when(i >= 2)
        def _():
            pl.semaphore_wait(credit, 1)
        part_copy(i).start()

    @pl.when((i >= 1) & (i <= nb))
    def _():
        m = i - 1
        s = lax.rem(m, 2)
        s4 = lax.rem(m, NP)
        copy = part_copy(m)
        copy.wait_send()
        copy.wait_recv()
        osum[lax.rem(m, NO)] = acc[s, pl.ds(0, 2)] + dl[s, pl.ds(0, 2)]
        kept = (chip == 0) & (lax.rem(m, RS) == R0)
        for c, full in ((0, True), (1, False)):
            @pl.when((chip == c) & (m >= NP) if c else (chip == c) & (m >= NP) & (lax.rem(m - NP + RS, RS) != R0))
            def _():
                sum_copy(m - NP, full).wait_send()

        @pl.when(kept)
        def _():
            rps[...] = acc[s, pl.ds(2, 2)] + dl[s, pl.ds(2, 2)]

        @pl.when(jnp.logical_not(kept))
        def _():
            ps[s4] = acc[s, pl.ds(2, 2)] + dl[s, pl.ds(2, 2)]

        @pl.when(m < nb - 2)
        def _():
            pl.semaphore_signal(credit, inc=1, device_id={'cp': peer}, device_id_type=MESH)

        @pl.when((chip == 0) & (lax.rem(m, RS) != R0))
        def _():
            sum_copy(m, True).start()

        @pl.when(chip == 1)
        def _():
            @pl.when(lax.rem(m, RS) == R0)
            def _():
                ret_copy(m).start()
            sum_copy(m, False).start()

    @pl.when((chip == 0) & (i >= RLAG) & (i < nb + RLAG) & (lax.rem(i - RLAG + RS, RS) == R0))
    def _():
        m = i - RLAG
        ret_copy(m).wait_recv()

        @pl.when(m >= RS)
        def _():
            for w in range(2):
                fin_copy(m - RS, w).wait_send()
        results(fin, rps, (), ret, (m // RS,))
        for w in range(2):
            fin_copy(m, w).start()

    @pl.when(i >= LAG)
    def _():
        m = i - LAG
        back = (chip == 1) & (lax.rem(m, RS) == R0)
        before = (chip == 1) & (lax.rem(m - 1 + RS, RS) == R0)

        @pl.when(back)
        def _():
            ret_copy(m).wait_send()

        @pl.when((m >= 1) & jnp.logical_not(before))
        def _():
            for w in range(2):
                out_copy(m - 1, w).wait()

        @pl.when(jnp.logical_not(back))
        def _():
            for c, full in ((0, False), (1, True)):
                @pl.when(chip == c)
                def _():
                    sum_copy(m, full).wait_recv()
                    n = pl.ds(0, 2 if full else 1)
                    copy = pltpu.make_async_copy(rl_hbm.at[m, n], buf.at[n], buf_sem)
                    copy.start()
                    copy.wait()
            results(stage, osum, (lax.rem(m, NO),), buf, ())
            for w in range(2):
                out_copy(m, w).start()

    @pl.when(i == nb + LAG - 1)
    def _():
        for w in range(2):
            out_copy(nb - 1, w).wait()
        for c, full in ((0, True), (1, False)):
            @pl.when(chip == c)
            def _():
                for m in range(nb - NP, nb):
                    if c == 1 or m % RS != R0:
                        sum_copy(m, full).wait_send()
        returned = range(R0, nb, RS)

        @pl.when(chip == 0)
        def _():
            for w in range(2):
                fin_copy(returned[-1], w).wait_send()

        @pl.when(chip == 1)
        def _():
            for m in returned:
                for w in range(2):
                    fin_copy(m, w).wait_recv()

        @pl.loop(0, ng)
        def _(j):
            for w in range(2):
                peer_copy(j, w).wait_send()
            for c, full in ((0, False), (1, True)):
                @pl.when(chip == c)
                def _():
                    for w in range(2):
                        x_copy(j, w, full).wait_send()
                        fwd_copy(j, w, not full).wait_send()


def _finish(*refs):
    for src, dst in zip(refs[:3], refs[3:]):
        dst[...] = src[...]


def solution(mesh):
    def local(q, k, v, do, o, lse):
        b, t, hq, d = q.shape
        hkv = k.shape[2]
        grp = hq // hkv
        scale = d ** -0.5
        ng = b // GB
        nr = len(range(R0, b, RS))
        assert (b - 1) % RS != R0 and RLAG <= RS
        heads = lambda x: jnp.transpose(x, (0, 2, 1, 3))
        q, do, o = (heads(x) for x in (q, do, o))
        lse = jnp.transpose(lse, (1, 0, 2))

        last = b - 1
        big = pl.BlockSpec((1, hq, t, d), lambda i: (jnp.minimum(i, last), 0, 0, 0))
        anyspec = pl.BlockSpec(memory_space=pl.ANY)
        dma = pltpu.SemaphoreType.DMA
        flops = 9 * b * hq * 5 * 2 * C * C * d
        shapes = [jax.ShapeDtypeStruct((b, hq, t, d), BF16),
                  jax.ShapeDtypeStruct((b, t, hkv, d), BF16),
                  jax.ShapeDtypeStruct((b, t, hkv, d), BF16)]
        dq, dk, dv, _ = pl.pallas_call(
            functools.partial(_kernel, b, hkv, grp, scale),
            grid=(b + LAG,),
            in_specs=[big, big, big,
                      pl.BlockSpec((hq, 8, t), lambda i: (0, jnp.minimum(i, last) // 8, 0)),
                      anyspec, anyspec],
            out_specs=[big, anyspec, anyspec, anyspec],
            out_shape=[*shapes, jax.ShapeDtypeStruct((b, 2, hkv, 2, C, d), F32)],
            scratch_shapes=[
                pltpu.VMEM((b, 4, t, hkv, d), BF16),
                pltpu.VMEM((b, 4, t, hkv, d), BF16),
                pltpu.VMEM((2, 4, hkv, t, d), BF16),
                pltpu.VMEM((2, 8, hkv, 2, C, d), F32),
                pltpu.VMEM((2, 4, hkv, 2, C, d), F32),
                pltpu.VMEM((NP, 2, hkv, 2, C, d), F32),
                pltpu.VMEM((NO, 2, hkv, 2, C, d), F32),
                pltpu.VMEM((2, hkv, 2, C, d), F32),
                pltpu.VMEM((nr, 2, hkv, 2, C, d), F32),
                pltpu.VMEM((2, hkv, 2, C, d), F32),
                pltpu.VMEM((2, t, hkv, d), BF16),
                pltpu.VMEM((2, t, hkv, d), BF16),
                pltpu.VMEM((2, hkv, d, grp * C), BF16),
                pltpu.VMEM((2, hkv, d, grp * C), BF16),
                pltpu.VMEM((2, hkv, d, grp * C), F32),
                pltpu.VMEM((2, hkv, 1, grp * C), F32),
                pltpu.VMEM((2, hkv, 1, grp * C), F32),
                dma((ng, 2)), dma((ng, 2)), dma((ng, 2)), dma((ng, 2)), dma((ng, 2)), dma((ng, 2)), dma((ng, 2)),
                dma((2,)), dma((2,)), dma((NP,)), dma((b,)), dma(()),
                dma((2,)), dma((2,)), dma((nr,)), dma((2,)), dma((nr, 2)), pltpu.SemaphoreType.REGULAR,
            ],
            compiler_params=pltpu.CompilerParams(
                dimension_semantics=('arbitrary',), collective_id=0, has_side_effects=True,
                vmem_limit_bytes=67043328),
            cost_estimate=pl.CostEstimate(flops=flops, bytes_accessed=4 * q.size * 2, transcendentals=0),
        )(q, do, o, lse, k, v)

        two = [pl.BlockSpec((2, *x.shape[1:]), lambda i: (i, 0, 0, 0)) for x in shapes]
        dq, dk, dv = pl.pallas_call(
            _finish, grid=(b // 2,), in_specs=two, out_specs=two, out_shape=shapes,
            compiler_params=pltpu.CompilerParams(dimension_semantics=('arbitrary',)),
        )(dq, dk, dv)
        return heads(dq), dk, dv

    spec = P('data', 'cp')
    return jax.shard_map(local, mesh=mesh, in_specs=(spec, spec, spec, spec, spec, P('data', None, 'cp')),
                         out_specs=(spec, spec, spec), check_vma=False)
```

```python
import functools
import jax
import jax.numpy as jnp
from jax import lax
from jax.experimental import pallas as pl
from jax.experimental.pallas import tpu as pltpu
from jax.sharding import PartitionSpec as P

F32 = jnp.float32
BF16 = jnp.bfloat16
MESH = pl.DeviceIdType.MESH

C = 128
GB = 4
NP = 4
LAG = 7
NO = 8
AHEAD = 3
RS, R0 = 8, 2
RLAG = 6
NL = 3

OWN, PARTNER, PEER, DIAG = 0, 1, 2, 3


def _dot(a, b):
    return lax.dot_general(a, b, (((1,), (0,)), ((), ())), preferred_element_type=F32)


def _kernel(nb, hkv, grp, scale,
            q_ref, do_ref, o_ref, lse_ref, k_hbm, v_hbm,
            dq_ref, dk_hbm, dv_hbm, rl_hbm, ol_hbm, pl_hbm,
            kl, vl, kd, acc, dl, ps, osum, buf, ret, rps, fin, stage, qt, dot_, dqt, lse_s, del_s,
            loc_sem, xs_sem, xr_sem, es_sem, er_sem, fs_sem, fr_sem,
            ds_sem, dr_sem, ps_sem, pr_sem, buf_sem, os_sem, rs_sem, rr_sem, ts_sem, tr_sem, tail_sem, credit):
    i = pl.program_id(0)
    r = lax.axis_index('cp')
    chip = r // 2
    odd = lax.rem(r, 2)
    peer = r + 1 - 2 * odd
    partner = lax.rem(r + 2, 4)
    ng = nb // GB
    rows = grp * C

    def kv(which):
        return (k_hbm, kl) if which == 0 else (v_hbm, vl)

    def local_copy(j, w):
        src, dst = kv(w)
        b = pl.ds(j * GB, GB)
        return pltpu.make_async_copy(src.at[b], dst.at[b, OWN], loc_sem.at[j, w])

    def peer_copy(j, w):
        src, dst = kv(w)
        b = pl.ds(j * GB, GB)
        return pltpu.make_async_remote_copy(src.at[b], dst.at[b, PEER], es_sem.at[j, w], er_sem.at[j, w],
                                            device_id={'cp': peer}, device_id_type=MESH)

    def x_copy(j, w, full):
        src, dst = kv(w)
        b = pl.ds(j * GB, GB)
        t = pl.ds(0, 2 * C if full else C)
        return pltpu.make_async_remote_copy(src.at[b, t], dst.at[b, PARTNER, t], xs_sem.at[j, w], xr_sem.at[j, w],
                                            device_id={'cp': partner}, device_id_type=MESH)

    def fwd_copy(j, w, full):
        _, dst = kv(w)
        b = pl.ds(j * GB, GB)
        t = pl.ds(0, 2 * C if full else C)
        return pltpu.make_async_remote_copy(dst.at[b, PARTNER, t], dst.at[b, DIAG, t], fs_sem.at[j, w], fr_sem.at[j, w],
                                            device_id={'cp': peer}, device_id_type=MESH)

    def part_copy(m):
        s = lax.rem(m, 2)
        return pltpu.make_async_remote_copy(acc.at[s, pl.ds(4, 4)], dl.at[s], ds_sem.at[s], dr_sem.at[s],
                                            device_id={'cp': peer}, device_id_type=MESH)

    def sum_copy(m, full):
        s = lax.rem(m, NP)
        n = pl.ds(0, 2 if full else 1)
        return pltpu.make_async_remote_copy(ps.at[s, n], rl_hbm.at[m, n], ps_sem.at[s], pr_sem.at[m],
                                            device_id={'cp': partner}, device_id_type=MESH)

    def ret_copy(m):
        n = m // RS
        return pltpu.make_async_remote_copy(osum.at[lax.rem(m, NO)], ret.at[n], rs_sem.at[lax.rem(n, 2)], rr_sem.at[n],
                                            device_id={'cp': partner}, device_id_type=MESH)

    def fin_copy(m, w):
        dst = (dk_hbm, dv_hbm)[w]
        return pltpu.make_async_remote_copy(fin.at[w], dst.at[m], ts_sem.at[w], tr_sem.at[m // RS, w],
                                            device_id={'cp': partner}, device_id_type=MESH)

    def out_copy(m, w):
        dst = (dk_hbm, dv_hbm)[w]
        return pltpu.make_async_copy(stage.at[w], dst.at[m], os_sem.at[w])

    def tail_copies(m):
        n = m - (nb - NL)
        return (pltpu.make_async_copy(osum.at[lax.rem(m, NO)], ol_hbm.at[n], tail_sem.at[n, 0]),
                pltpu.make_async_copy(ps.at[lax.rem(m, NP)], pl_hbm.at[n], tail_sem.at[n, 1]))

    def results(dst, a, a_slot, b_, b_slot):
        for sg in range(2):
            for w in range(2):
                x = [a[(*a_slot, sg, g, w)] + b_[(*b_slot, sg, g, w)] for g in range(hkv)]
                if w == 0:
                    x = [y * scale for y in x]
                dst[w, pl.ds(sg * C, C)] = jnp.stack(x, axis=1).astype(BF16)

    def forward(j):
        for c, full in ((0, True), (1, False)):
            @pl.when(chip == c)
            def _():
                for w in range(2):
                    x_copy(j, w, full).wait_recv()
                    fwd_copy(j, w, full).start()

    @pl.when(i == 0)
    def _():
        barrier = pltpu.get_barrier_semaphore()
        for other in (peer, partner):
            pl.semaphore_signal(barrier, inc=1, device_id={'cp': other}, device_id_type=MESH)
        pl.semaphore_wait(barrier, 2)

        @pl.loop(0, ng)
        def _(j):
            for c, full in ((0, False), (1, True)):
                @pl.when((chip == c) if c == 0 else ((chip == c) & (j < AHEAD)))
                def _():
                    for w in range(2):
                        x_copy(j, w, full).start()
            for w in range(2):
                local_copy(j, w).start()
                peer_copy(j, w).start()
        buf[...] = jnp.zeros_like(buf)
        forward(0)

    @pl.when(i < nb)
    def _():
        b = i
        slot = lax.rem(i, 2)
        j = i // GB

        @pl.when(lax.rem(i, GB) == 0)
        def _():
            for w in range(2):
                local_copy(j, w).wait()
                peer_copy(j, w).wait_recv()
            for c, full in ((0, True), (1, False)):
                @pl.when(chip == c)
                def _():
                    for w in range(2):
                        fwd_copy(j, w, full).wait_recv()

        @pl.when((lax.rem(i, GB) == 0) & (chip == 1) & (j >= 1) & (j < ng - AHEAD + 1))
        def _():
            for w in range(2):
                x_copy(j + AHEAD - 1, w, True).start()

        @pl.when((lax.rem(i, GB) == GB // 2) & (i < nb - GB))
        def _():
            forward(j + 1)

        acc[slot] = jnp.zeros(acc.shape[1:], F32)
        dqt[...] = jnp.zeros_like(dqt)
        row = lax.rem(i, 8)
        for w in range(2):
            for sec in range(4):
                kd[w, sec] = jnp.transpose(kv(w)[1][b, sec], (1, 0, 2))
        for g in range(hkv):
            for hh in range(grp):
                h = g * grp + hh
                lanes = pl.ds(hh * C, C)
                lse_row = lse_ref[h, pl.ds(row, 1), :]
                for sg in range(2):
                    tok = pl.ds(sg * C, C)
                    dob = do_ref[0, h, tok, :]
                    qt[sg, g, :, lanes] = q_ref[0, h, tok, :].T
                    dot_[sg, g, :, lanes] = dob.T
                    prod = dob.astype(F32) * o_ref[0, h, tok, :].astype(F32)
                    del_s[sg, g, :, lanes] = jnp.sum(prod.T, axis=0, keepdims=True)
                    lse_s[sg, g, :, lanes] = lse_row[:, sg * C:(sg + 1) * C]

        def pair(qs, ks, shift):
            sec, half = ks // 2, lax.rem(ks, 2)
            keys = pl.ds(pl.multiple_of(half * C, C), C)
            toks = pl.ds(pl.multiple_of(qs * C, C), C)
            for g in range(hkv):
                k = kd[0, sec, g, keys, :]
                v = kd[1, sec, g, keys, :]
                heads = pl.ds(g * grp, grp)
                s = _dot(k, qt[qs, g])
                p = jnp.exp(s * scale - lse_s[qs, g])
                if shift is not None:
                    ki = lax.broadcasted_iota(jnp.int32, (C, rows), 0)
                    qi = lax.bitwise_and(lax.broadcasted_iota(jnp.int32, (C, rows), 1), C - 1)
                    p = jnp.where(ki <= qi + shift, p, 0.0)
                dp = _dot(v, dot_[qs, g])
                ds = (p * (dp - del_s[qs, g])).astype(BF16)
                acc[slot, ks, g, 1] += _dot(p.astype(BF16), do_ref[0, heads, toks, :].reshape(rows, C))
                acc[slot, ks, g, 0] += _dot(ds, q_ref[0, heads, toks, :].reshape(rows, C))
                dqt[qs, g] += _dot(k.T, ds)

        @pl.loop(0, 3)
        def _(t):
            pair((t + 1) // 2, t // 2, C * lax.rem(t, 2))

        @pl.loop(0, 2)
        def _(t):
            pair(1 - odd * (1 - t), 4 + t * (1 - odd), None)

        @pl.loop(0, 4)
        def _(t):
            u = (1 - chip) * t + chip * 2 * (t // 2)
            pair((1 - chip) + chip * lax.rem(t, 2), 2 + lax.rem(u, 2) + 4 * (u // 2), None)

        for g in range(hkv):
            for hh in range(grp):
                for sg in range(2):
                    x = dqt[sg, g, :, pl.ds(hh * C, C)].T
                    dq_ref[0, g * grp + hh, pl.ds(sg * C, C), :] = (x * scale).astype(BF16)

        @pl.when(i >= 2)
        def _():
            pl.semaphore_wait(credit, 1)
        part_copy(i).start()

    @pl.when((i >= 1) & (i <= nb))
    def _():
        m = i - 1
        s = lax.rem(m, 2)
        s4 = lax.rem(m, NP)
        copy = part_copy(m)
        copy.wait_send()
        copy.wait_recv()
        osum[lax.rem(m, NO)] = acc[s, pl.ds(0, 2)] + dl[s, pl.ds(0, 2)]
        kept = (chip == 0) & (lax.rem(m, RS) == R0)
        for c, full in ((0, True), (1, False)):
            @pl.when((chip == c) & (m >= NP) if c else (chip == c) & (m >= NP) & (lax.rem(m - NP + RS, RS) != R0))
            def _():
                sum_copy(m - NP, full).wait_send()

        @pl.when(kept)
        def _():
            rps[...] = acc[s, pl.ds(2, 2)] + dl[s, pl.ds(2, 2)]

        @pl.when(jnp.logical_not(kept))
        def _():
            ps[s4] = acc[s, pl.ds(2, 2)] + dl[s, pl.ds(2, 2)]

        @pl.when(m < nb - 2)
        def _():
            pl.semaphore_signal(credit, inc=1, device_id={'cp': peer}, device_id_type=MESH)

        @pl.when(m >= nb - NL)
        def _():
            for copy in tail_copies(m):
                copy.start()

        @pl.when((chip == 0) & (lax.rem(m, RS) != R0) & (m < nb - NL))
        def _():
            sum_copy(m, True).start()

        @pl.when((chip == 1) & (m < nb - NL))
        def _():
            @pl.when(lax.rem(m, RS) == R0)
            def _():
                ret_copy(m).start()
            sum_copy(m, False).start()

    @pl.when((chip == 0) & (i >= RLAG) & (i < nb - NL + RLAG) & (lax.rem(i - RLAG + RS, RS) == R0))
    def _():
        m = i - RLAG
        ret_copy(m).wait_recv()

        @pl.when(m >= RS)
        def _():
            for w in range(2):
                fin_copy(m - RS, w).wait_send()
        results(fin, rps, (), ret, (m // RS,))
        for w in range(2):
            fin_copy(m, w).start()

    @pl.when(i >= LAG)
    def _():
        m = i - LAG
        back = (chip == 1) & (lax.rem(m, RS) == R0)
        before = (chip == 1) & (lax.rem(m - 1 + RS, RS) == R0)

        @pl.when(back)
        def _():
            ret_copy(m).wait_send()

        @pl.when((m >= 1) & jnp.logical_not(before))
        def _():
            for w in range(2):
                out_copy(m - 1, w).wait()

        @pl.when(jnp.logical_not(back))
        def _():
            for c, full in ((0, False), (1, True)):
                @pl.when(chip == c)
                def _():
                    sum_copy(m, full).wait_recv()
                    n = pl.ds(0, 2 if full else 1)
                    copy = pltpu.make_async_copy(rl_hbm.at[m, n], buf.at[n], buf_sem)
                    copy.start()
                    copy.wait()
            results(stage, osum, (lax.rem(m, NO),), buf, ())
            for w in range(2):
                out_copy(m, w).start()

    @pl.when(i == nb - NL + LAG - 1)
    def _():
        for w in range(2):
            out_copy(nb - NL - 1, w).wait()
        for c, full in ((0, True), (1, False)):
            @pl.when(chip == c)
            def _():
                for m in range(nb - NP, nb - NL):
                    if c == 1 or m % RS != R0:
                        sum_copy(m, full).wait_send()
        for m in range(nb - NL, nb):
            for copy in tail_copies(m):
                copy.wait()
        returned = range(R0, nb - NL, RS)

        @pl.when(chip == 0)
        def _():
            for w in range(2):
                fin_copy(returned[-1], w).wait_send()

        @pl.when(chip == 1)
        def _():
            for m in returned:
                for w in range(2):
                    fin_copy(m, w).wait_recv()

        @pl.loop(0, ng)
        def _(j):
            for w in range(2):
                peer_copy(j, w).wait_send()
            for c, full in ((0, False), (1, True)):
                @pl.when(chip == c)
                def _():
                    for w in range(2):
                        x_copy(j, w, full).wait_send()
                        fwd_copy(j, w, not full).wait_send()


def _finish(*refs):
    for src, dst in zip(refs[:3], refs[3:]):
        dst[...] = src[...]


def _last(scale, dk_in, dv_in, own_ref, got_ref, dk_ref, dv_ref):
    n = pl.program_id(0)
    hkv = own_ref.shape[2]
    for sg in range(2):
        for w, dst in enumerate((dk_ref, dv_ref)):
            x = [own_ref[n, sg, g, w] + got_ref[n, sg, g, w] for g in range(hkv)]
            if w == 0:
                x = [y * scale for y in x]
            dst[0, pl.ds(sg * C, C)] = jnp.stack(x, axis=1).astype(BF16)


def solution(mesh):
    swap = [(r, (r + 2) % 4) for r in range(4)]

    def local(q, k, v, do, o, lse):
        b, t, hq, d = q.shape
        hkv = k.shape[2]
        grp = hq // hkv
        scale = d ** -0.5
        ng = b // GB
        nr = len(range(R0, b - NL, RS))
        assert (b - NL - 1) % RS != R0 and RLAG <= RS and NL <= NP
        heads = lambda x: jnp.transpose(x, (0, 2, 1, 3))
        q, do, o = (heads(x) for x in (q, do, o))
        lse = jnp.transpose(lse, (1, 0, 2))

        last = b - 1
        big = pl.BlockSpec((1, hq, t, d), lambda i: (jnp.minimum(i, last), 0, 0, 0))
        anyspec = pl.BlockSpec(memory_space=pl.ANY)
        dma = pltpu.SemaphoreType.DMA
        flops = 9 * b * hq * 5 * 2 * C * C * d
        shapes = [jax.ShapeDtypeStruct((b, hq, t, d), BF16),
                  jax.ShapeDtypeStruct((b, t, hkv, d), BF16),
                  jax.ShapeDtypeStruct((b, t, hkv, d), BF16)]
        dq, dk, dv, _, own, sums = pl.pallas_call(
            functools.partial(_kernel, b, hkv, grp, scale),
            grid=(b - NL + LAG,),
            in_specs=[big, big, big,
                      pl.BlockSpec((hq, 8, t), lambda i: (0, jnp.minimum(i, last) // 8, 0)),
                      anyspec, anyspec],
            out_specs=[big, *[anyspec] * 5],
            out_shape=[*shapes, *(jax.ShapeDtypeStruct((n, 2, hkv, 2, C, d), F32) for n in (b, NL, NL))],
            scratch_shapes=[
                pltpu.VMEM((b, 4, t, hkv, d), BF16),
                pltpu.VMEM((b, 4, t, hkv, d), BF16),
                pltpu.VMEM((2, 4, hkv, t, d), BF16),
                pltpu.VMEM((2, 8, hkv, 2, C, d), F32),
                pltpu.VMEM((2, 4, hkv, 2, C, d), F32),
                pltpu.VMEM((NP, 2, hkv, 2, C, d), F32),
                pltpu.VMEM((NO, 2, hkv, 2, C, d), F32),
                pltpu.VMEM((2, hkv, 2, C, d), F32),
                pltpu.VMEM((nr, 2, hkv, 2, C, d), F32),
                pltpu.VMEM((2, hkv, 2, C, d), F32),
                pltpu.VMEM((2, t, hkv, d), BF16),
                pltpu.VMEM((2, t, hkv, d), BF16),
                pltpu.VMEM((2, hkv, d, grp * C), BF16),
                pltpu.VMEM((2, hkv, d, grp * C), BF16),
                pltpu.VMEM((2, hkv, d, grp * C), F32),
                pltpu.VMEM((2, hkv, 1, grp * C), F32),
                pltpu.VMEM((2, hkv, 1, grp * C), F32),
                dma((ng, 2)), dma((ng, 2)), dma((ng, 2)), dma((ng, 2)), dma((ng, 2)), dma((ng, 2)), dma((ng, 2)),
                dma((2,)), dma((2,)), dma((NP,)), dma((b,)), dma(()),
                dma((2,)), dma((2,)), dma((nr,)), dma((2,)), dma((nr, 2)), dma((NL, 2)), pltpu.SemaphoreType.REGULAR,
            ],
            compiler_params=pltpu.CompilerParams(
                dimension_semantics=('arbitrary',), collective_id=0, has_side_effects=True,
                vmem_limit_bytes=67043328),
            cost_estimate=pl.CostEstimate(flops=flops, bytes_accessed=4 * q.size * 2, transcendentals=0),
        )(q, do, o, lse, k, v)

        got = lax.ppermute(sums, 'cp', swap)
        two = [pl.BlockSpec((2, *x.shape[1:]), lambda i: (i, 0, 0, 0)) for x in shapes]
        dq, dk, dv = pl.pallas_call(
            _finish, grid=(b // 2,), in_specs=two, out_specs=two, out_shape=shapes,
            compiler_params=pltpu.CompilerParams(dimension_semantics=('arbitrary',)),
            cost_estimate=pl.CostEstimate(flops=10**8, bytes_accessed=4 * q.size, transcendentals=0),
        )(dq, dk, dv)
        one = pl.BlockSpec(memory_space=pltpu.VMEM)
        out = pl.BlockSpec((1, t, hkv, d), lambda i: (b - NL + i, 0, 0, 0))
        dk, dv = pl.pallas_call(
            functools.partial(_last, scale), grid=(NL,), in_specs=[anyspec, anyspec, one, one],
            out_specs=[out, out], out_shape=shapes[1:], input_output_aliases={0: 0, 1: 1},
            compiler_params=pltpu.CompilerParams(dimension_semantics=('arbitrary',)),
        )(dk, dv, own, got)
        return heads(dq), dk, dv

    spec = P('data', 'cp')
    return jax.shard_map(local, mesh=mesh, in_specs=(spec, spec, spec, spec, spec, P('data', None, 'cp')),
                         out_specs=(spec, spec, spec), check_vma=False)
```

```python
import functools
import jax
import jax.numpy as jnp
from jax import lax
from jax.experimental import pallas as pl
from jax.experimental.pallas import tpu as pltpu
from jax.sharding import PartitionSpec as P

F32 = jnp.float32
BF16 = jnp.bfloat16
MESH = pl.DeviceIdType.MESH

C = 128
GB = 4
NP = 4
LAG = 8
NO = 8
AHEAD = 3
RS, R0 = 8, 2
RLAG = 6
NL = 3

OWN, PARTNER, PEER, DIAG = 0, 1, 2, 3


def _dot(a, b):
    return lax.dot_general(a, b, (((1,), (0,)), ((), ())), preferred_element_type=F32)


def _kernel(nb, hkv, grp, scale,
            q_ref, do_ref, o_ref, lse_ref, k_hbm, v_hbm,
            dq_ref, dk_hbm, dv_hbm, rl_hbm, ol_hbm, pl_hbm,
            kl, vl, raw, acc, dl, ps, osum, buf, ret, rps, fin, stage, qt, dot_, dqt, lse_s, del_s,
            loc_sem, xs_sem, xr_sem, es_sem, er_sem, fs_sem, fr_sem,
            ds_sem, dr_sem, ps_sem, pr_sem, buf_sem, os_sem, rs_sem, rr_sem, ts_sem, tr_sem, tail_sem, credit):
    i = pl.program_id(0)
    r = lax.axis_index('cp')
    chip = r // 2
    odd = lax.rem(r, 2)
    peer = r + 1 - 2 * odd
    partner = lax.rem(r + 2, 4)
    ng = nb // GB
    rows = grp * C

    def kv(which):
        return (k_hbm, kl) if which == 0 else (v_hbm, vl)

    def local_copy(j, w):
        n = lax.rem(j, 2)
        return pltpu.make_async_copy(kv(w)[0].at[pl.ds(j * GB, GB)], raw.at[n, w], loc_sem.at[n, w])

    def peer_copy(j, w):
        _, dst = kv(w)
        b = pl.ds(j * GB, GB)
        return pltpu.make_async_remote_copy(dst.at[b, OWN], dst.at[b, PEER], es_sem.at[j, w], er_sem.at[j, w],
                                            device_id={'cp': peer}, device_id_type=MESH)

    def x_copy(j, w, full):
        _, dst = kv(w)
        b = pl.ds(j * GB, GB)
        t = pl.ds(0, 2 * C if full else C)
        return pltpu.make_async_remote_copy(dst.at[b, OWN, :, t], dst.at[b, PARTNER, :, t], xs_sem.at[j, w], xr_sem.at[j, w],
                                            device_id={'cp': partner}, device_id_type=MESH)

    def fwd_copy(j, w, full):
        _, dst = kv(w)
        b = pl.ds(j * GB, GB)
        t = pl.ds(0, 2 * C if full else C)
        return pltpu.make_async_remote_copy(dst.at[b, PARTNER, :, t], dst.at[b, DIAG, :, t], fs_sem.at[j, w], fr_sem.at[j, w],
                                            device_id={'cp': peer}, device_id_type=MESH)

    def part_copy(m):
        s = lax.rem(m, 2)
        return pltpu.make_async_remote_copy(acc.at[s, pl.ds(4, 4)], dl.at[s], ds_sem.at[s], dr_sem.at[s],
                                            device_id={'cp': peer}, device_id_type=MESH)

    def sum_copy(m, full):
        s = lax.rem(m, NP)
        n = pl.ds(0, 2 if full else 1)
        return pltpu.make_async_remote_copy(ps.at[s, n], rl_hbm.at[m, n], ps_sem.at[s], pr_sem.at[m],
                                            device_id={'cp': partner}, device_id_type=MESH)

    def ret_copy(m):
        n = m // RS
        return pltpu.make_async_remote_copy(osum.at[lax.rem(m, NO)], ret.at[n], rs_sem.at[lax.rem(n, 2)], rr_sem.at[n],
                                            device_id={'cp': partner}, device_id_type=MESH)

    def fin_copy(m, w):
        dst = (dk_hbm, dv_hbm)[w]
        return pltpu.make_async_remote_copy(fin.at[w], dst.at[m], ts_sem.at[w], tr_sem.at[m // RS, w],
                                            device_id={'cp': partner}, device_id_type=MESH)

    def out_copy(m, w):
        dst = (dk_hbm, dv_hbm)[w]
        return pltpu.make_async_copy(stage.at[w], dst.at[m], os_sem.at[w])

    def buf_copy(m, full):
        n = pl.ds(0, 2 if full else 1)
        return pltpu.make_async_copy(rl_hbm.at[m, n], buf.at[n], buf_sem)

    def tail_copies(m):
        n = m - (nb - NL)
        return (pltpu.make_async_copy(osum.at[lax.rem(m, NO)], ol_hbm.at[n], tail_sem.at[n, 0]),
                pltpu.make_async_copy(ps.at[lax.rem(m, NP)], pl_hbm.at[n], tail_sem.at[n, 1]))

    def results(dst, a, a_slot, b_, b_slot):
        for sg in range(2):
            for w in range(2):
                x = [a[(*a_slot, sg, g, w)] + b_[(*b_slot, sg, g, w)] for g in range(hkv)]
                if w == 0:
                    x = [y * scale for y in x]
                dst[w, pl.ds(sg * C, C)] = jnp.stack(x, axis=1).astype(BF16)

    def forward(j):
        for c, full in ((0, True), (1, False)):
            @pl.when(chip == c)
            def _():
                for w in range(2):
                    x_copy(j, w, full).wait_recv()
                    fwd_copy(j, w, full).start()

    @pl.when(i == 0)
    def _():
        barrier = pltpu.get_barrier_semaphore()
        for other in (peer, partner):
            pl.semaphore_signal(barrier, inc=1, device_id={'cp': other}, device_id_type=MESH)
        pl.semaphore_wait(barrier, 2)

        for j in range(2):
            for w in range(2):
                local_copy(j, w).start()

        @pl.loop(0, ng)
        def _(j):
            for w in range(2):
                local_copy(j, w).wait()
                for n in range(GB):
                    kv(w)[1][j * GB + n, OWN] = jnp.transpose(raw[lax.rem(j, 2), w, n], (1, 0, 2))
            for c, full in ((0, False), (1, True)):
                @pl.when((chip == c) if c == 0 else ((chip == c) & (j < AHEAD)))
                def _():
                    for w in range(2):
                        x_copy(j, w, full).start()
            for w in range(2):
                peer_copy(j, w).start()

            @pl.when(j < ng - 2)
            def _():
                for w in range(2):
                    local_copy(j + 2, w).start()
        buf[...] = jnp.zeros_like(buf)
        forward(0)

    @pl.when(i >= LAG)
    def _():
        m = i - LAG

        @pl.when((chip == 0) | (lax.rem(m, RS) != R0))
        def _():
            for c, full in ((0, False), (1, True)):
                @pl.when(chip == c)
                def _():
                    sum_copy(m, full).wait_recv()
                    buf_copy(m, full).start()

    @pl.when(i < nb)
    def _():
        b = i
        slot = lax.rem(i, 2)
        j = i // GB

        @pl.when(lax.rem(i, GB) == 0)
        def _():
            for w in range(2):
                peer_copy(j, w).wait_recv()
            for c, full in ((0, True), (1, False)):
                @pl.when(chip == c)
                def _():
                    for w in range(2):
                        fwd_copy(j, w, full).wait_recv()

        @pl.when((lax.rem(i, GB) == 0) & (chip == 1) & (j >= 1) & (j < ng - AHEAD + 1))
        def _():
            for w in range(2):
                x_copy(j + AHEAD - 1, w, True).start()

        @pl.when((lax.rem(i, GB) == GB // 2) & (i < nb - GB))
        def _():
            forward(j + 1)

        acc[slot] = jnp.zeros(acc.shape[1:], F32)
        dqt[...] = jnp.zeros_like(dqt)
        row = lax.rem(i, 8)
        for g in range(hkv):
            for hh in range(grp):
                h = g * grp + hh
                lanes = pl.ds(hh * C, C)
                lse_row = lse_ref[h, pl.ds(row, 1), :]
                for sg in range(2):
                    tok = pl.ds(sg * C, C)
                    do_t = do_ref[0, h, tok, :].T
                    qt[sg, g, :, lanes] = q_ref[0, h, tok, :].T
                    dot_[sg, g, :, lanes] = do_t
                    prod = do_t.astype(F32) * o_ref[0, h, tok, :].T.astype(F32)
                    del_s[sg, g, :, lanes] = jnp.sum(prod, axis=0, keepdims=True)
                    lse_s[sg, g, :, lanes] = lse_row[:, sg * C:(sg + 1) * C]

        def block(qs, kss, shifts):
            toks = pl.ds(pl.multiple_of(qs * C, C), C)
            for g in range(hkv):
                def keys(src):
                    x = [src[b, ks // 2, g, pl.ds(pl.multiple_of(lax.rem(ks, 2) * C, C), C), :] for ks in kss]
                    return x[0] if len(x) == 1 else jnp.concatenate(x, axis=0)

                k = keys(kl)
                heads = pl.ds(g * grp, grp)
                p = jnp.exp(_dot(k, qt[qs, g]) * scale - lse_s[qs, g])
                if shifts is not None:
                    ki = lax.broadcasted_iota(jnp.int32, (C, rows), 0)
                    qi = lax.bitwise_and(lax.broadcasted_iota(jnp.int32, (C, rows), 1), C - 1)
                    x = [jnp.where(ki <= qi + shift, p[n * C:(n + 1) * C], 0.0) for n, shift in enumerate(shifts)]
                    p = x[0] if len(x) == 1 else jnp.concatenate(x, axis=0)
                ds = (p * (_dot(keys(vl), dot_[qs, g]) - del_s[qs, g])).astype(BF16)
                dv = _dot(p.astype(BF16), do_ref[0, heads, toks, :].reshape(rows, C))
                dk = _dot(ds, q_ref[0, heads, toks, :].reshape(rows, C))
                for n, ks in enumerate(kss):
                    acc[slot, ks, g, 0] += dk[n * C:(n + 1) * C]
                    acc[slot, ks, g, 1] += dv[n * C:(n + 1) * C]
                dqt[qs, g] += _dot(k.T, ds)

        @pl.loop(0, 2)
        def _(t):
            block(1 - t * odd, (4 * t * (1 - odd), 1 + t * (4 - odd)), (C * (1 - t * odd), C * t))

        block(odd, (4 * odd,), (C * odd,))

        @pl.loop(0, 2)
        def _(t):
            block((1 - chip) + chip * t, (2 + 4 * t * (1 - chip), (1 - chip) * (3 + 4 * t) + chip * 6), None)

        @pl.when(i >= 2)
        def _():
            pl.semaphore_wait(credit, 1)
        part_copy(i).start()

        for g in range(hkv):
            for hh in range(grp):
                for sg in range(2):
                    x = dqt[sg, g, :, pl.ds(hh * C, C)].T
                    dq_ref[0, g * grp + hh, pl.ds(sg * C, C), :] = (x * scale).astype(BF16)

    @pl.when((i >= 1) & (i <= nb))
    def _():
        m = i - 1
        s = lax.rem(m, 2)
        s4 = lax.rem(m, NP)
        copy = part_copy(m)
        copy.wait_send()
        copy.wait_recv()
        osum[lax.rem(m, NO)] = acc[s, pl.ds(0, 2)] + dl[s, pl.ds(0, 2)]
        kept = (chip == 0) & (lax.rem(m, RS) == R0)
        for c, full in ((0, True), (1, False)):
            @pl.when((chip == c) & (m >= NP) if c else (chip == c) & (m >= NP) & (lax.rem(m - NP + RS, RS) != R0))
            def _():
                sum_copy(m - NP, full).wait_send()

        @pl.when(kept)
        def _():
            rps[...] = acc[s, pl.ds(2, 2)] + dl[s, pl.ds(2, 2)]

        @pl.when(jnp.logical_not(kept))
        def _():
            ps[s4] = acc[s, pl.ds(2, 2)] + dl[s, pl.ds(2, 2)]

        @pl.when(m < nb - 2)
        def _():
            pl.semaphore_signal(credit, inc=1, device_id={'cp': peer}, device_id_type=MESH)

        @pl.when(m >= nb - NL)
        def _():
            for copy in tail_copies(m):
                copy.start()

        @pl.when((chip == 0) & (lax.rem(m, RS) != R0) & (m < nb - NL))
        def _():
            sum_copy(m, True).start()

        @pl.when((chip == 1) & (m < nb - NL))
        def _():
            @pl.when(lax.rem(m, RS) == R0)
            def _():
                ret_copy(m).start()
            sum_copy(m, False).start()

    @pl.when((chip == 0) & (i >= RLAG) & (i < nb - NL + RLAG) & (lax.rem(i - RLAG + RS, RS) == R0))
    def _():
        m = i - RLAG
        ret_copy(m).wait_recv()

        @pl.when(m >= RS)
        def _():
            for w in range(2):
                fin_copy(m - RS, w).wait_send()
        results(fin, rps, (), ret, (m // RS,))
        for w in range(2):
            fin_copy(m, w).start()

    @pl.when(i >= LAG)
    def _():
        m = i - LAG
        back = (chip == 1) & (lax.rem(m, RS) == R0)
        before = (chip == 1) & (lax.rem(m - 1 + RS, RS) == R0)

        @pl.when(back)
        def _():
            ret_copy(m).wait_send()

        @pl.when((m >= 1) & jnp.logical_not(before))
        def _():
            for w in range(2):
                out_copy(m - 1, w).wait()

        @pl.when(jnp.logical_not(back))
        def _():
            for c, full in ((0, False), (1, True)):
                @pl.when(chip == c)
                def _():
                    buf_copy(m, full).wait()
            results(stage, osum, (lax.rem(m, NO),), buf, ())
            for w in range(2):
                out_copy(m, w).start()

    @pl.when(i == nb - NL + LAG - 1)
    def _():
        for w in range(2):
            out_copy(nb - NL - 1, w).wait()
        for c, full in ((0, True), (1, False)):
            @pl.when(chip == c)
            def _():
                for m in range(nb - NP, nb - NL):
                    if c == 1 or m % RS != R0:
                        sum_copy(m, full).wait_send()
        for m in range(nb - NL, nb):
            for copy in tail_copies(m):
                copy.wait()
        returned = range(R0, nb - NL, RS)

        @pl.when(chip == 0)
        def _():
            for w in range(2):
                fin_copy(returned[-1], w).wait_send()

        @pl.when(chip == 1)
        def _():
            for m in returned:
                for w in range(2):
                    fin_copy(m, w).wait_recv()

        @pl.loop(0, ng)
        def _(j):
            for w in range(2):
                peer_copy(j, w).wait_send()
            for c, full in ((0, False), (1, True)):
                @pl.when(chip == c)
                def _():
                    for w in range(2):
                        x_copy(j, w, full).wait_send()
                        fwd_copy(j, w, not full).wait_send()


def _finish(*refs):
    for src, dst in zip(refs[:3], refs[3:]):
        dst[...] = src[...]


def _last(scale, dk_in, dv_in, own_ref, got_ref, dk_ref, dv_ref):
    n = pl.program_id(0)
    hkv = own_ref.shape[2]
    for sg in range(2):
        for w, dst in enumerate((dk_ref, dv_ref)):
            x = [own_ref[n, sg, g, w] + got_ref[n, sg, g, w] for g in range(hkv)]
            if w == 0:
                x = [y * scale for y in x]
            dst[0, pl.ds(sg * C, C)] = jnp.stack(x, axis=1).astype(BF16)


def solution(mesh):
    swap = [(r, (r + 2) % 4) for r in range(4)]

    def local(q, k, v, do, o, lse):
        b, t, hq, d = q.shape
        hkv = k.shape[2]
        grp = hq // hkv
        scale = d ** -0.5
        ng = b // GB
        nr = len(range(R0, b - NL, RS))
        assert (b - NL - 1) % RS != R0 and RLAG <= RS and NL <= NP
        heads = lambda x: jnp.transpose(x, (0, 2, 1, 3))
        q, do, o = (heads(x) for x in (q, do, o))
        lse = jnp.transpose(lse, (1, 0, 2))

        last = b - 1
        big = pl.BlockSpec((1, hq, t, d), lambda i: (jnp.minimum(i, last), 0, 0, 0))
        anyspec = pl.BlockSpec(memory_space=pl.ANY)
        dma = pltpu.SemaphoreType.DMA
        flops = 9 * b * hq * 5 * 2 * C * C * d
        shapes = [jax.ShapeDtypeStruct((b, hq, t, d), BF16),
                  jax.ShapeDtypeStruct((b, t, hkv, d), BF16),
                  jax.ShapeDtypeStruct((b, t, hkv, d), BF16)]
        dq, dk, dv, _, own, sums = pl.pallas_call(
            functools.partial(_kernel, b, hkv, grp, scale),
            grid=(b - NL + LAG,),
            in_specs=[big, big, big,
                      pl.BlockSpec((hq, 8, t), lambda i: (0, jnp.minimum(i, last) // 8, 0)),
                      anyspec, anyspec],
            out_specs=[big, *[anyspec] * 5],
            out_shape=[*shapes, *(jax.ShapeDtypeStruct((n, 2, hkv, 2, C, d), F32) for n in (b, NL, NL))],
            scratch_shapes=[
                pltpu.VMEM((b, 4, hkv, t, d), BF16),
                pltpu.VMEM((b, 4, hkv, t, d), BF16),
                pltpu.VMEM((2, 2, GB, t, hkv, d), BF16),
                pltpu.VMEM((2, 8, hkv, 2, C, d), F32),
                pltpu.VMEM((2, 4, hkv, 2, C, d), F32),
                pltpu.VMEM((NP, 2, hkv, 2, C, d), F32),
                pltpu.VMEM((NO, 2, hkv, 2, C, d), F32),
                pltpu.VMEM((2, hkv, 2, C, d), F32),
                pltpu.VMEM((nr, 2, hkv, 2, C, d), F32),
                pltpu.VMEM((2, hkv, 2, C, d), F32),
                pltpu.VMEM((2, t, hkv, d), BF16),
                pltpu.VMEM((2, t, hkv, d), BF16),
                pltpu.VMEM((2, hkv, d, grp * C), BF16),
                pltpu.VMEM((2, hkv, d, grp * C), BF16),
                pltpu.VMEM((2, hkv, d, grp * C), F32),
                pltpu.VMEM((2, hkv, 1, grp * C), F32),
                pltpu.VMEM((2, hkv, 1, grp * C), F32),
                dma((2, 2)), dma((ng, 2)), dma((ng, 2)), dma((ng, 2)), dma((ng, 2)), dma((ng, 2)), dma((ng, 2)),
                dma((2,)), dma((2,)), dma((NP,)), dma((b,)), dma(()),
                dma((2,)), dma((2,)), dma((nr,)), dma((2,)), dma((nr, 2)), dma((NL, 2)), pltpu.SemaphoreType.REGULAR,
            ],
            compiler_params=pltpu.CompilerParams(
                dimension_semantics=('arbitrary',), collective_id=0, has_side_effects=True,
                vmem_limit_bytes=67043328),
            cost_estimate=pl.CostEstimate(flops=flops, bytes_accessed=4 * q.size * 2, transcendentals=0),
        )(q, do, o, lse, k, v)

        got = lax.ppermute(sums, 'cp', swap)
        two = [pl.BlockSpec((2, *x.shape[1:]), lambda i: (i, 0, 0, 0)) for x in shapes]
        dq, dk, dv = pl.pallas_call(
            _finish, grid=(b // 2,), in_specs=two, out_specs=two, out_shape=shapes,
            compiler_params=pltpu.CompilerParams(dimension_semantics=('arbitrary',)),
            cost_estimate=pl.CostEstimate(flops=10**8, bytes_accessed=4 * q.size, transcendentals=0),
        )(dq, dk, dv)
        one = pl.BlockSpec(memory_space=pltpu.VMEM)
        out = pl.BlockSpec((1, t, hkv, d), lambda i: (b - NL + i, 0, 0, 0))
        dk, dv = pl.pallas_call(
            functools.partial(_last, scale), grid=(NL,), in_specs=[anyspec, anyspec, one, one],
            out_specs=[out, out], out_shape=shapes[1:], input_output_aliases={0: 0, 1: 1},
            compiler_params=pltpu.CompilerParams(dimension_semantics=('arbitrary',)),
        )(dk, dv, own, got)
        return heads(dq), dk, dv

    spec = P('data', 'cp')
    return jax.shard_map(local, mesh=mesh, in_specs=(spec, spec, spec, spec, spec, P('data', None, 'cp')),
                         out_specs=(spec, spec, spec), check_vma=False)
```

```python
import functools
import jax
import jax.numpy as jnp
from jax import lax
from jax.experimental import pallas as pl
from jax.experimental.pallas import tpu as pltpu
from jax.sharding import PartitionSpec as P

F32 = jnp.float32
BF16 = jnp.bfloat16
MESH = pl.DeviceIdType.MESH

C = 128
GB = 4
NP = 4
LAG = 8
NO = 8
AHEAD = 3
RS, R0 = 5, 1
RLAG = 5
NL = 3

OWN, PARTNER, PEER, DIAG = 0, 1, 2, 3


def _dot(a, b):
    return lax.dot_general(a, b, (((1,), (0,)), ((), ())), preferred_element_type=F32)


def _kernel(nb, hkv, grp, scale,
            q_ref, do_ref, o_ref, lse_ref, k_hbm, v_hbm,
            dq_ref, dk_hbm, dv_hbm, rl_hbm, ol_hbm, pl_hbm,
            kl, vl, raw, acc, dl, ps, osum, buf, ret, rps, fin, stage, qt, dot_, dqt, lse_s, del_s,
            loc_sem, xs_sem, xr_sem, es_sem, er_sem, fs_sem, fr_sem,
            ds_sem, dr_sem, ps_sem, pr_sem, buf_sem, os_sem, rs_sem, rr_sem, ts_sem, tr_sem, tail_sem, credit):
    i = pl.program_id(0)
    r = lax.axis_index('cp')
    chip = r // 2
    odd = lax.rem(r, 2)
    peer = r + 1 - 2 * odd
    partner = lax.rem(r + 2, 4)
    ng = nb // GB
    rows = grp * C
    first_late = nb - NL * (2 - chip)
    first_kept = nb - NL * (1 + chip)

    def returned(m):
        return (lax.rem(m + RS, RS) == R0) & (m < nb - 2 * NL)

    def kv(which):
        return (k_hbm, kl) if which == 0 else (v_hbm, vl)

    def local_copy(j, w):
        n = lax.rem(j, 2)
        return pltpu.make_async_copy(kv(w)[0].at[pl.ds(j * GB, GB)], raw.at[n, w], loc_sem.at[n, w])

    def peer_copy(j, w):
        _, dst = kv(w)
        b = pl.ds(j * GB, GB)
        return pltpu.make_async_remote_copy(dst.at[b, OWN], dst.at[b, PEER], es_sem.at[j, w], er_sem.at[j, w],
                                            device_id={'cp': peer}, device_id_type=MESH)

    def x_copy(j, w, full):
        _, dst = kv(w)
        b = pl.ds(j * GB, GB)
        t = pl.ds(0, 2 * C if full else C)
        return pltpu.make_async_remote_copy(dst.at[b, OWN, :, t], dst.at[b, PARTNER, :, t], xs_sem.at[j, w], xr_sem.at[j, w],
                                            device_id={'cp': partner}, device_id_type=MESH)

    def fwd_copy(j, w, full):
        _, dst = kv(w)
        b = pl.ds(j * GB, GB)
        t = pl.ds(0, 2 * C if full else C)
        return pltpu.make_async_remote_copy(dst.at[b, PARTNER, :, t], dst.at[b, DIAG, :, t], fs_sem.at[j, w], fr_sem.at[j, w],
                                            device_id={'cp': peer}, device_id_type=MESH)

    def part_copy(m):
        s = lax.rem(m, 2)
        return pltpu.make_async_remote_copy(acc.at[s, pl.ds(4, 4)], dl.at[s], ds_sem.at[s], dr_sem.at[s],
                                            device_id={'cp': peer}, device_id_type=MESH)

    def sum_copy(m, full):
        s = lax.rem(m, NP)
        n = pl.ds(0, 2 if full else 1)
        return pltpu.make_async_remote_copy(ps.at[s, n], rl_hbm.at[m, n], ps_sem.at[s], pr_sem.at[m],
                                            device_id={'cp': partner}, device_id_type=MESH)

    def ret_copy(m):
        n = m // RS
        return pltpu.make_async_remote_copy(osum.at[lax.rem(m, NO)], ret.at[n], rs_sem.at[lax.rem(n, 2)], rr_sem.at[n],
                                            device_id={'cp': partner}, device_id_type=MESH)

    def fin_copy(m, w):
        dst = (dk_hbm, dv_hbm)[w]
        return pltpu.make_async_remote_copy(fin.at[w], dst.at[m], ts_sem.at[w], tr_sem.at[m // RS, w],
                                            device_id={'cp': partner}, device_id_type=MESH)

    def out_copy(m, w):
        dst = (dk_hbm, dv_hbm)[w]
        return pltpu.make_async_copy(stage.at[w], dst.at[m], os_sem.at[w])

    def buf_copy(m, full):
        n = pl.ds(0, 2 if full else 1)
        return pltpu.make_async_copy(rl_hbm.at[m, n], buf.at[n], buf_sem)

    def late(m, act):
        n = m - (nb - 2 * NL)
        slot = lax.rem(m, NP)

        @pl.when(m >= first_late)
        def _():
            act(pltpu.make_async_copy(osum.at[lax.rem(m, NO)], ol_hbm.at[n], tail_sem.at[n, 0]))

        @pl.when((chip == 0) & (m >= first_kept))
        def _():
            act(pltpu.make_async_copy(ps.at[slot], pl_hbm.at[n - NL], tail_sem.at[n, 1]))

        @pl.when((chip == 1) & (m >= first_kept))
        def _():
            one, at = pl.ds(0, 1), pl.ds(1 - n // NL, 1)
            act(pltpu.make_async_copy(ps.at[slot, one], pl_hbm.at[lax.rem(n, NL), at], tail_sem.at[n, 1]))

    def results(dst, a, a_slot, b_, b_slot):
        for sg in range(2):
            for w in range(2):
                x = [a[(*a_slot, sg, g, w)] + b_[(*b_slot, sg, g, w)] for g in range(hkv)]
                if w == 0:
                    x = [y * scale for y in x]
                dst[w, pl.ds(sg * C, C)] = jnp.stack(x, axis=1).astype(BF16)

    def forward(j):
        for c, full in ((0, True), (1, False)):
            @pl.when(chip == c)
            def _():
                for w in range(2):
                    x_copy(j, w, full).wait_recv()
                    fwd_copy(j, w, full).start()

    @pl.when(i == 0)
    def _():
        barrier = pltpu.get_barrier_semaphore()
        for other in (peer, partner):
            pl.semaphore_signal(barrier, inc=1, device_id={'cp': other}, device_id_type=MESH)
        pl.semaphore_wait(barrier, 2)

        for j in range(2):
            for w in range(2):
                local_copy(j, w).start()

        @pl.loop(0, ng)
        def _(j):
            for w in range(2):
                local_copy(j, w).wait()
                for n in range(GB):
                    kv(w)[1][j * GB + n, OWN] = jnp.transpose(raw[lax.rem(j, 2), w, n], (1, 0, 2))
                for c, full in ((0, False), (1, True)):
                    @pl.when((chip == c) if c == 0 else ((chip == c) & (j < AHEAD)))
                    def _():
                        x_copy(j, w, full).start()
                peer_copy(j, w).start()

            @pl.when(j < ng - 2)
            def _():
                for w in range(2):
                    local_copy(j + 2, w).start()
        buf[...] = jnp.zeros_like(buf)
        forward(0)

    @pl.when(i >= LAG)
    def _():
        m = i - LAG

        @pl.when((m < first_late) & ((chip == 0) | jnp.logical_not(returned(m))))
        def _():
            for c, full in ((0, False), (1, True)):
                @pl.when(chip == c)
                def _():
                    sum_copy(m, full).wait_recv()
                    buf_copy(m, full).start()

    @pl.when(i < nb)
    def _():
        b = i
        slot = lax.rem(i, 2)
        j = i // GB

        @pl.when(lax.rem(i, GB) == 0)
        def _():
            for w in range(2):
                peer_copy(j, w).wait_recv()
            for c, full in ((0, True), (1, False)):
                @pl.when(chip == c)
                def _():
                    for w in range(2):
                        fwd_copy(j, w, full).wait_recv()

        @pl.when((lax.rem(i, GB) == 0) & (chip == 1) & (j >= 1) & (j < ng - AHEAD + 1))
        def _():
            for w in range(2):
                x_copy(j + AHEAD - 1, w, True).start()

        @pl.when((lax.rem(i, GB) == GB // 2) & (i < nb - GB))
        def _():
            forward(j + 1)

        acc[slot] = jnp.zeros(acc.shape[1:], F32)
        dqt[...] = jnp.zeros_like(dqt)
        row = lax.rem(i, 8)
        for g in range(hkv):
            for hh in range(grp):
                h = g * grp + hh
                lanes = pl.ds(hh * C, C)
                lse_row = lse_ref[h, pl.ds(row, 1), :]
                for sg in range(2):
                    tok = pl.ds(sg * C, C)
                    do_t = do_ref[0, h, tok, :].T
                    qt[sg, g, :, lanes] = q_ref[0, h, tok, :].T
                    dot_[sg, g, :, lanes] = do_t
                    prod = do_t.astype(F32) * o_ref[0, h, tok, :].T.astype(F32)
                    del_s[sg, g, :, lanes] = jnp.sum(prod, axis=0, keepdims=True)
                    lse_s[sg, g, :, lanes] = lse_row[:, sg * C:(sg + 1) * C]

        def block(qs, kss, shifts):
            toks = pl.ds(pl.multiple_of(qs * C, C), C)
            for g in range(hkv):
                def keys(src):
                    x = [src[b, ks // 2, g, pl.ds(pl.multiple_of(lax.rem(ks, 2) * C, C), C), :] for ks in kss]
                    return x[0] if len(x) == 1 else jnp.concatenate(x, axis=0)

                k = keys(kl)
                heads = pl.ds(g * grp, grp)
                p = jnp.exp(_dot(k, qt[qs, g]) * scale - lse_s[qs, g])
                if shifts is not None:
                    ki = lax.broadcasted_iota(jnp.int32, (C, rows), 0)
                    qi = lax.bitwise_and(lax.broadcasted_iota(jnp.int32, (C, rows), 1), C - 1)
                    x = [jnp.where(ki <= qi + shift, p[n * C:(n + 1) * C], 0.0) for n, shift in enumerate(shifts)]
                    p = x[0] if len(x) == 1 else jnp.concatenate(x, axis=0)
                ds = (p * (_dot(keys(vl), dot_[qs, g]) - del_s[qs, g])).astype(BF16)
                dv = _dot(p.astype(BF16), do_ref[0, heads, toks, :].reshape(rows, C))
                dk = _dot(ds, q_ref[0, heads, toks, :].reshape(rows, C))
                for n, ks in enumerate(kss):
                    acc[slot, ks, g, 0] += dk[n * C:(n + 1) * C]
                    acc[slot, ks, g, 1] += dv[n * C:(n + 1) * C]
                dqt[qs, g] += _dot(k.T, ds)

        @pl.loop(0, 2)
        def _(t):
            block(1 - t * odd, (4 * t * (1 - odd), 1 + t * (4 - odd)), (C * (1 - t * odd), C * t))

        block(odd, (4 * odd,), (C * odd,))

        @pl.loop(0, 2)
        def _(t):
            block((1 - chip) + chip * t, (2 + 4 * t * (1 - chip), (1 - chip) * (3 + 4 * t) + chip * 6), None)

        @pl.when(i >= 2)
        def _():
            pl.semaphore_wait(credit, 1)
        part_copy(i).start()

        for g in range(hkv):
            for hh in range(grp):
                for sg in range(2):
                    x = dqt[sg, g, :, pl.ds(hh * C, C)].T
                    dq_ref[0, g * grp + hh, pl.ds(sg * C, C), :] = (x * scale).astype(BF16)

    @pl.when((i >= 1) & (i <= nb))
    def _():
        m = i - 1
        s = lax.rem(m, 2)
        s4 = lax.rem(m, NP)
        copy = part_copy(m)
        copy.wait_send()
        copy.wait_recv()
        osum[lax.rem(m, NO)] = acc[s, pl.ds(0, 2)] + dl[s, pl.ds(0, 2)]
        kept = (chip == 0) & returned(m)
        for c, full in ((0, True), (1, False)):
            @pl.when((chip == c) & (m >= NP) &
                     ((m - NP < first_kept) if c else jnp.logical_not(returned(m - NP))))
            def _():
                sum_copy(m - NP, full).wait_send()

        @pl.when(kept)
        def _():
            rps[...] = acc[s, pl.ds(2, 2)] + dl[s, pl.ds(2, 2)]

        @pl.when(jnp.logical_not(kept))
        def _():
            ps[s4] = acc[s, pl.ds(2, 2)] + dl[s, pl.ds(2, 2)]

        @pl.when(m < nb - 2)
        def _():
            pl.semaphore_signal(credit, inc=1, device_id={'cp': peer}, device_id_type=MESH)

        @pl.when(m >= 1)
        def _():
            late(m - 1, lambda copy: copy.wait())
        late(m, lambda copy: copy.start())

        @pl.when((chip == 0) & jnp.logical_not(returned(m)) & (m < first_kept))
        def _():
            sum_copy(m, True).start()

        @pl.when(chip == 1)
        def _():
            @pl.when(returned(m))
            def _():
                ret_copy(m).start()

            @pl.when(m < first_kept)
            def _():
                sum_copy(m, False).start()

    @pl.when((chip == 0) & (i >= RLAG) & returned(i - RLAG))
    def _():
        m = i - RLAG
        ret_copy(m).wait_recv()

        @pl.when(m >= RS)
        def _():
            for w in range(2):
                fin_copy(m - RS, w).wait_send()
        results(fin, rps, (), ret, (m // RS,))
        for w in range(2):
            fin_copy(m, w).start()

    @pl.when(i >= LAG)
    def _():
        m = i - LAG
        back = (chip == 1) & returned(m)
        before = (chip == 1) & returned(m - 1)

        @pl.when(back)
        def _():
            ret_copy(m).wait_send()

        @pl.when((m >= 1) & (m - 1 < first_late) & jnp.logical_not(before))
        def _():
            for w in range(2):
                out_copy(m - 1, w).wait()

        @pl.when((m < first_late) & jnp.logical_not(back))
        def _():
            for c, full in ((0, False), (1, True)):
                @pl.when(chip == c)
                def _():
                    buf_copy(m, full).wait()
            results(stage, osum, (lax.rem(m, NO),), buf, ())
            for w in range(2):
                out_copy(m, w).start()

    @pl.when(i == nb - NL + LAG - 1)
    def _():
        late(nb - 1, lambda copy: copy.wait())
        all_returned = range(R0, nb - 2 * NL, RS)

        @pl.when(chip == 1)
        def _():
            for w in range(2):
                out_copy(nb - NL - 1, w).wait()

        @pl.when(chip == 0)
        def _():
            for m in range(nb - NP, nb - NL):
                sum_copy(m, True).wait_send()

        @pl.when(chip == 0)
        def _():
            for w in range(2):
                fin_copy(all_returned[-1], w).wait_send()

        @pl.when(chip == 1)
        def _():
            for m in all_returned:
                for w in range(2):
                    fin_copy(m, w).wait_recv()

        @pl.loop(0, ng)
        def _(j):
            for w in range(2):
                peer_copy(j, w).wait_send()
            for c, full in ((0, False), (1, True)):
                @pl.when(chip == c)
                def _():
                    for w in range(2):
                        x_copy(j, w, full).wait_send()
                        fwd_copy(j, w, not full).wait_send()


def _finish(*refs):
    for src, dst in zip(refs[:3], refs[3:]):
        dst[...] = src[...]


def _last(nb, scale, dk_in, dv_in, own_ref, got_ref, dk_hbm, dv_hbm, stage, sem):
    chip = lax.axis_index('cp') // 2
    hkv = own_ref.shape[2]
    outs = (dk_hbm, dv_hbm)

    def copies(n):
        return [pltpu.make_async_copy(stage.at[n, w], outs[w].at[nb - 2 * NL + n], sem.at[n, w]) for w in range(2)]

    def batch(n, terms):
        for sg in range(2):
            for w in range(2):
                x = [own_ref[n, sg, g, w] for g in range(hkv)]
                if terms[sg] is not None:
                    x = [y + got_ref[(*terms[sg], g, w)] for g, y in enumerate(x)]
                if w == 0:
                    x = [y * scale for y in x]
                stage[n, w, pl.ds(sg * C, C)] = jnp.stack(x, axis=1).astype(BF16)
        for copy in copies(n):
            copy.start()

    for c in range(2):
        @pl.when(chip == c)
        def _():
            for n in range(NL * c, 2 * NL):
                if n < NL:
                    batch(n, ((n, 1), None))
                else:
                    batch(n, ((n - NL, 0), (n - NL, 1) if c else None))
            for n in range(NL * c, 2 * NL):
                for copy in copies(n):
                    copy.wait()


def solution(mesh):
    swap = [(r, (r + 2) % 4) for r in range(4)]

    def local(q, k, v, do, o, lse):
        b, t, hq, d = q.shape
        hkv = k.shape[2]
        grp = hq // hkv
        scale = d ** -0.5
        ng = b // GB
        nr = len(range(R0, b - 2 * NL, RS))
        assert RLAG <= RS and NL <= NP and 2 * NL <= NO
        heads = lambda x: jnp.transpose(x, (0, 2, 1, 3))
        q, do, o = (heads(x) for x in (q, do, o))
        lse = jnp.transpose(lse, (1, 0, 2))

        last = b - 1
        big = pl.BlockSpec((1, hq, t, d), lambda i: (jnp.minimum(i, last), 0, 0, 0))
        anyspec = pl.BlockSpec(memory_space=pl.ANY)
        dma = pltpu.SemaphoreType.DMA
        flops = 9 * b * hq * 5 * 2 * C * C * d
        shapes = [jax.ShapeDtypeStruct((b, hq, t, d), BF16),
                  jax.ShapeDtypeStruct((b, t, hkv, d), BF16),
                  jax.ShapeDtypeStruct((b, t, hkv, d), BF16)]
        dq, dk, dv, _, own, sums = pl.pallas_call(
            functools.partial(_kernel, b, hkv, grp, scale),
            grid=(b - NL + LAG,),
            in_specs=[big, big, big,
                      pl.BlockSpec((hq, 8, t), lambda i: (0, jnp.minimum(i, last) // 8, 0)),
                      anyspec, anyspec],
            out_specs=[big, *[anyspec] * 5],
            out_shape=[*shapes, *(jax.ShapeDtypeStruct((n, 2, hkv, 2, C, d), F32) for n in (b, 2 * NL, NL))],
            scratch_shapes=[
                pltpu.VMEM((b, 4, hkv, t, d), BF16),
                pltpu.VMEM((b, 4, hkv, t, d), BF16),
                pltpu.VMEM((2, 2, GB, t, hkv, d), BF16),
                pltpu.VMEM((2, 8, hkv, 2, C, d), F32),
                pltpu.VMEM((2, 4, hkv, 2, C, d), F32),
                pltpu.VMEM((NP, 2, hkv, 2, C, d), F32),
                pltpu.VMEM((NO, 2, hkv, 2, C, d), F32),
                pltpu.VMEM((2, hkv, 2, C, d), F32),
                pltpu.VMEM((nr, 2, hkv, 2, C, d), F32),
                pltpu.VMEM((2, hkv, 2, C, d), F32),
                pltpu.VMEM((2, t, hkv, d), BF16),
                pltpu.VMEM((2, t, hkv, d), BF16),
                pltpu.VMEM((2, hkv, d, grp * C), BF16),
                pltpu.VMEM((2, hkv, d, grp * C), BF16),
                pltpu.VMEM((2, hkv, d, grp * C), F32),
                pltpu.VMEM((2, hkv, 1, grp * C), F32),
                pltpu.VMEM((2, hkv, 1, grp * C), F32),
                dma((2, 2)), dma((ng, 2)), dma((ng, 2)), dma((ng, 2)), dma((ng, 2)), dma((ng, 2)), dma((ng, 2)),
                dma((2,)), dma((2,)), dma((NP,)), dma((b,)), dma(()),
                dma((2,)), dma((2,)), dma((nr,)), dma((2,)), dma((nr, 2)), dma((2 * NL, 2)), pltpu.SemaphoreType.REGULAR,
            ],
            compiler_params=pltpu.CompilerParams(
                dimension_semantics=('arbitrary',), collective_id=0, has_side_effects=True,
                vmem_limit_bytes=67043328),
            cost_estimate=pl.CostEstimate(flops=flops, bytes_accessed=4 * q.size * 2, transcendentals=0),
        )(q, do, o, lse, k, v)

        got = lax.ppermute(sums, 'cp', swap)
        two = [pl.BlockSpec((2, *x.shape[1:]), lambda i: (i, 0, 0, 0)) for x in shapes]
        dq, dk, dv = pl.pallas_call(
            _finish, grid=(b // 2,), in_specs=two, out_specs=two, out_shape=shapes,
            compiler_params=pltpu.CompilerParams(dimension_semantics=('arbitrary',)),
            cost_estimate=pl.CostEstimate(flops=10**8, bytes_accessed=4 * q.size, transcendentals=0),
        )(dq, dk, dv)
        one = pl.BlockSpec(memory_space=pltpu.VMEM)
        dk, dv = pl.pallas_call(
            functools.partial(_last, b, scale), in_specs=[anyspec, anyspec, one, one],
            out_specs=[anyspec, anyspec], out_shape=shapes[1:], input_output_aliases={0: 0, 1: 1},
            scratch_shapes=[pltpu.VMEM((2 * NL, 2, t, hkv, d), BF16), dma((2 * NL, 2))],
        )(dk, dv, own, got)
        return heads(dq), dk, dv

    spec = P('data', 'cp')
    return jax.shard_map(local, mesh=mesh, in_specs=(spec, spec, spec, spec, spec, P('data', None, 'cp')),
                         out_specs=(spec, spec, spec), check_vma=False)
```

```python
import functools
import jax
import jax.numpy as jnp
from jax import lax
from jax.experimental import pallas as pl
from jax.experimental.pallas import tpu as pltpu
from jax.sharding import PartitionSpec as P

F32 = jnp.float32
BF16 = jnp.bfloat16
MESH = pl.DeviceIdType.MESH

C = 128
GB = 4
NP = 4
LAG = 11
NO = 11
AHEAD = 3
RS, R0 = 5, 1
RLAG = 10
NL = 3

OWN, PARTNER, PEER, DIAG = 0, 1, 2, 3


def _dot(a, b):
    return lax.dot_general(a, b, (((1,), (0,)), ((), ())), preferred_element_type=F32)


def _kernel(nb, hkv, grp, scale,
            q_ref, do_ref, o_ref, lse_ref, k_hbm, v_hbm,
            dq_ref, dk_hbm, dv_hbm, rl_hbm, ol_hbm, pl_hbm,
            kl, vl, raw, acc, dl, ps, osum, buf, ret, rps, fin, stage, qt, dot_, dqt, lse_s, del_s,
            loc_sem, xs_sem, xr_sem, es_sem, er_sem, fs_sem, fr_sem,
            ds_sem, dr_sem, ps_sem, pr_sem, buf_sem, os_sem, rs_sem, rr_sem, ts_sem, tr_sem, tail_sem, credit):
    i = pl.program_id(0)
    r = lax.axis_index('cp')
    chip = r // 2
    odd = lax.rem(r, 2)
    peer = r + 1 - 2 * odd
    partner = lax.rem(r + 2, 4)
    ng = nb // GB
    rows = grp * C
    first_late = nb - NL * (2 - chip)
    first_kept = nb - NL * (1 + chip)

    def returned(m):
        return (lax.rem(m + RS, RS) == R0) & (m < nb - 2 * NL)

    def kv(which):
        return (k_hbm, kl) if which == 0 else (v_hbm, vl)

    def local_copy(j, w):
        return pltpu.make_async_copy(kv(w)[0].at[pl.ds(j * GB, GB)], raw.at[w], loc_sem.at[w])

    def peer_copy(j, w):
        _, dst = kv(w)
        b = pl.ds(j * GB, GB)
        return pltpu.make_async_remote_copy(dst.at[b, OWN], dst.at[b, PEER], es_sem.at[j, w], er_sem.at[j, w],
                                            device_id={'cp': peer}, device_id_type=MESH)

    def x_copy(j, w, full):
        _, dst = kv(w)
        b = pl.ds(j * GB, GB)
        t = pl.ds(0, 2 * C if full else C)
        return pltpu.make_async_remote_copy(dst.at[b, OWN, :, t], dst.at[b, PARTNER, :, t], xs_sem.at[j, w], xr_sem.at[j, w],
                                            device_id={'cp': partner}, device_id_type=MESH)

    def fwd_copy(j, w, full):
        _, dst = kv(w)
        b = pl.ds(j * GB, GB)
        t = pl.ds(0, 2 * C if full else C)
        return pltpu.make_async_remote_copy(dst.at[b, PARTNER, :, t], dst.at[b, DIAG, :, t], fs_sem.at[j, w], fr_sem.at[j, w],
                                            device_id={'cp': peer}, device_id_type=MESH)

    def part_copy(m):
        s = lax.rem(m, 2)
        return pltpu.make_async_remote_copy(acc.at[s, pl.ds(4, 4)], dl.at[s], ds_sem.at[s], dr_sem.at[s],
                                            device_id={'cp': peer}, device_id_type=MESH)

    def sum_copy(m, full):
        s = lax.rem(m, NP)
        n = pl.ds(0, 2 if full else 1)
        return pltpu.make_async_remote_copy(ps.at[s, n], rl_hbm.at[m, n], ps_sem.at[s], pr_sem.at[m],
                                            device_id={'cp': partner}, device_id_type=MESH)

    def ret_copy(m):
        n = m // RS
        return pltpu.make_async_remote_copy(osum.at[lax.rem(m, NO)], ret.at[n], rs_sem.at[lax.rem(n, 3)], rr_sem.at[n],
                                            device_id={'cp': partner}, device_id_type=MESH)

    def fin_copy(m, w):
        dst = (dk_hbm, dv_hbm)[w]
        return pltpu.make_async_remote_copy(fin.at[w], dst.at[m], ts_sem.at[w], tr_sem.at[m // RS, w],
                                            device_id={'cp': partner}, device_id_type=MESH)

    def out_copy(m, w):
        dst = (dk_hbm, dv_hbm)[w]
        return pltpu.make_async_copy(stage.at[w], dst.at[m], os_sem.at[w])

    def buf_copy(m, full):
        n = pl.ds(0, 2 if full else 1)
        return pltpu.make_async_copy(rl_hbm.at[m, n], buf.at[n], buf_sem)

    def late(m, act):
        n = m - (nb - 2 * NL)
        slot = lax.rem(m, NP)

        @pl.when(m >= first_late)
        def _():
            act(pltpu.make_async_copy(osum.at[lax.rem(m, NO)], ol_hbm.at[n], tail_sem.at[n, 0]))

        @pl.when((chip == 0) & (m >= first_kept))
        def _():
            act(pltpu.make_async_copy(ps.at[slot], pl_hbm.at[n - NL], tail_sem.at[n, 1]))

        @pl.when((chip == 1) & (m >= first_kept))
        def _():
            one, at = pl.ds(0, 1), pl.ds(1 - n // NL, 1)
            act(pltpu.make_async_copy(ps.at[slot, one], pl_hbm.at[lax.rem(n, NL), at], tail_sem.at[n, 1]))

    def results(dst, a, a_slot, b_, b_slot):
        for sg in range(2):
            for w in range(2):
                x = [a[(*a_slot, sg, g, w)] + b_[(*b_slot, sg, g, w)] for g in range(hkv)]
                if w == 0:
                    x = [y * scale for y in x]
                dst[w, pl.ds(sg * C, C)] = jnp.stack(x, axis=1).astype(BF16)

    def forward(j):
        for c, full in ((0, True), (1, False)):
            @pl.when(chip == c)
            def _():
                for w in range(2):
                    x_copy(j, w, full).wait_recv()
                    fwd_copy(j, w, full).start()

    @pl.when(i == 0)
    def _():
        barrier = pltpu.get_barrier_semaphore()
        for other in (peer, partner):
            pl.semaphore_signal(barrier, inc=1, device_id={'cp': other}, device_id_type=MESH)
        pl.semaphore_wait(barrier, 2)

        for w in range(2):
            local_copy(0, w).start()

        @pl.loop(0, ng)
        def _(j):
            for w in range(2):
                local_copy(j, w).wait()
                for n in range(GB):
                    kv(w)[1][j * GB + n, OWN] = jnp.transpose(raw[w, n], (1, 0, 2))

                @pl.when(j < ng - 1)
                def _():
                    local_copy(j + 1, w).start()
                for c, full in ((0, False), (1, True)):
                    @pl.when((chip == c) if c == 0 else ((chip == c) & (j < AHEAD)))
                    def _():
                        x_copy(j, w, full).start()
                peer_copy(j, w).start()

        buf[...] = jnp.zeros_like(buf)
        forward(0)

    @pl.when(i >= LAG)
    def _():
        m = i - LAG

        @pl.when((m < first_late) & ((chip == 0) | jnp.logical_not(returned(m))))
        def _():
            for c, full in ((0, False), (1, True)):
                @pl.when(chip == c)
                def _():
                    sum_copy(m, full).wait_recv()
                    buf_copy(m, full).start()

    @pl.when(i < nb)
    def _():
        b = i
        slot = lax.rem(i, 2)
        j = i // GB

        @pl.when(lax.rem(i, GB) == 0)
        def _():
            for w in range(2):
                peer_copy(j, w).wait_recv()
            for c, full in ((0, True), (1, False)):
                @pl.when(chip == c)
                def _():
                    for w in range(2):
                        fwd_copy(j, w, full).wait_recv()

        @pl.when((lax.rem(i, GB) == 0) & (chip == 1) & (j >= 1) & (j < ng - AHEAD + 1))
        def _():
            for w in range(2):
                x_copy(j + AHEAD - 1, w, True).start()

        @pl.when((lax.rem(i, GB) == GB // 2) & (i < nb - GB))
        def _():
            forward(j + 1)

        acc[slot] = jnp.zeros(acc.shape[1:], F32)
        dqt[...] = jnp.zeros_like(dqt)
        row = lax.rem(i, 8)
        for g in range(hkv):
            for hh in range(grp):
                h = g * grp + hh
                lanes = pl.ds(hh * C, C)
                lse_row = lse_ref[h, pl.ds(row, 1), :]
                for sg in range(2):
                    tok = pl.ds(sg * C, C)
                    do_t = do_ref[0, h, tok, :].T
                    qt[sg, g, :, lanes] = q_ref[0, h, tok, :].T
                    dot_[sg, g, :, lanes] = do_t
                    prod = do_t.astype(F32) * o_ref[0, h, tok, :].T.astype(F32)
                    del_s[sg, g, :, lanes] = jnp.sum(prod, axis=0, keepdims=True)
                    lse_s[sg, g, :, lanes] = lse_row[:, sg * C:(sg + 1) * C]

        def block(qs, kss, shifts):
            toks = pl.ds(pl.multiple_of(qs * C, C), C)
            for g in range(hkv):
                def keys(src):
                    x = [src[b, ks // 2, g, pl.ds(pl.multiple_of(lax.rem(ks, 2) * C, C), C), :] for ks in kss]
                    return x[0] if len(x) == 1 else jnp.concatenate(x, axis=0)

                k = keys(kl)
                heads = pl.ds(g * grp, grp)
                p = jnp.exp(_dot(k, qt[qs, g]) * scale - lse_s[qs, g])
                if shifts is not None:
                    ki = lax.broadcasted_iota(jnp.int32, (C, rows), 0)
                    qi = lax.bitwise_and(lax.broadcasted_iota(jnp.int32, (C, rows), 1), C - 1)
                    x = [jnp.where(ki <= qi + shift, p[n * C:(n + 1) * C], 0.0) for n, shift in enumerate(shifts)]
                    p = x[0] if len(x) == 1 else jnp.concatenate(x, axis=0)
                ds = (p * (_dot(keys(vl), dot_[qs, g]) - del_s[qs, g])).astype(BF16)
                dv = _dot(p.astype(BF16), do_ref[0, heads, toks, :].reshape(rows, C))
                dk = _dot(ds, q_ref[0, heads, toks, :].reshape(rows, C))
                for n, ks in enumerate(kss):
                    acc[slot, ks, g, 0] += dk[n * C:(n + 1) * C]
                    acc[slot, ks, g, 1] += dv[n * C:(n + 1) * C]
                dqt[qs, g] += _dot(k.T, ds)

        @pl.loop(0, 2)
        def _(t):
            block(1 - t * odd, (4 * t * (1 - odd), 1 + t * (4 - odd)), (C * (1 - t * odd), C * t))

        block(odd, (4 * odd,), (C * odd,))

        @pl.loop(0, 2)
        def _(t):
            block((1 - chip) + chip * t, (2 + 4 * t * (1 - chip), (1 - chip) * (3 + 4 * t) + chip * 6), None)

        @pl.when(i >= 2)
        def _():
            pl.semaphore_wait(credit, 1)
        part_copy(i).start()

        for g in range(hkv):
            for hh in range(grp):
                for sg in range(2):
                    x = dqt[sg, g, :, pl.ds(hh * C, C)].T
                    dq_ref[0, g * grp + hh, pl.ds(sg * C, C), :] = (x * scale).astype(BF16)

    @pl.when((i >= 1) & (i <= nb))
    def _():
        m = i - 1
        s = lax.rem(m, 2)
        s4 = lax.rem(m, NP)
        copy = part_copy(m)
        copy.wait_send()
        copy.wait_recv()
        osum[lax.rem(m, NO)] = acc[s, pl.ds(0, 2)] + dl[s, pl.ds(0, 2)]
        kept = (chip == 0) & returned(m)
        for c, full in ((0, True), (1, False)):
            @pl.when((chip == c) & (m >= NP) &
                     ((m - NP < first_kept) if c else jnp.logical_not(returned(m - NP))))
            def _():
                sum_copy(m - NP, full).wait_send()

        @pl.when(kept)
        def _():
            rps[lax.rem(m // RS, 2)] = acc[s, pl.ds(2, 2)] + dl[s, pl.ds(2, 2)]

        @pl.when(jnp.logical_not(kept))
        def _():
            ps[s4] = acc[s, pl.ds(2, 2)] + dl[s, pl.ds(2, 2)]

        @pl.when(m < nb - 2)
        def _():
            pl.semaphore_signal(credit, inc=1, device_id={'cp': peer}, device_id_type=MESH)

        @pl.when(m >= 1)
        def _():
            late(m - 1, lambda copy: copy.wait())
        late(m, lambda copy: copy.start())

        @pl.when((chip == 0) & jnp.logical_not(returned(m)) & (m < first_kept))
        def _():
            sum_copy(m, True).start()

        @pl.when(chip == 1)
        def _():
            @pl.when(returned(m))
            def _():
                ret_copy(m).start()

            @pl.when(m < first_kept)
            def _():
                sum_copy(m, False).start()

    @pl.when((chip == 0) & (i >= RLAG) & returned(i - RLAG))
    def _():
        m = i - RLAG
        ret_copy(m).wait_recv()

        @pl.when(m >= RS)
        def _():
            for w in range(2):
                fin_copy(m - RS, w).wait_send()
        results(fin, rps, (lax.rem(m // RS, 2),), ret, (m // RS,))
        for w in range(2):
            fin_copy(m, w).start()

    @pl.when(i >= LAG)
    def _():
        m = i - LAG
        back = (chip == 1) & returned(m)
        before = (chip == 1) & returned(m - 1)

        @pl.when(back)
        def _():
            ret_copy(m).wait_send()

        @pl.when((m >= 1) & (m - 1 < first_late) & jnp.logical_not(before))
        def _():
            for w in range(2):
                out_copy(m - 1, w).wait()

        @pl.when((m < first_late) & jnp.logical_not(back))
        def _():
            for c, full in ((0, False), (1, True)):
                @pl.when(chip == c)
                def _():
                    buf_copy(m, full).wait()
            results(stage, osum, (lax.rem(m, NO),), buf, ())
            for w in range(2):
                out_copy(m, w).start()

    @pl.when(i == nb - NL + LAG - 1)
    def _():
        late(nb - 1, lambda copy: copy.wait())
        all_returned = range(R0, nb - 2 * NL, RS)

        @pl.when(chip == 1)
        def _():
            for w in range(2):
                out_copy(nb - NL - 1, w).wait()

        @pl.when(chip == 0)
        def _():
            for m in range(nb - NP, nb - NL):
                sum_copy(m, True).wait_send()

        @pl.when(chip == 0)
        def _():
            for w in range(2):
                fin_copy(all_returned[-1], w).wait_send()

        @pl.when(chip == 1)
        def _():
            for m in all_returned:
                for w in range(2):
                    fin_copy(m, w).wait_recv()

        @pl.loop(0, ng)
        def _(j):
            for w in range(2):
                peer_copy(j, w).wait_send()
            for c, full in ((0, False), (1, True)):
                @pl.when(chip == c)
                def _():
                    for w in range(2):
                        x_copy(j, w, full).wait_send()
                        fwd_copy(j, w, not full).wait_send()


def _finish(*refs):
    for src, dst in zip(refs[:3], refs[3:]):
        dst[...] = src[...]


def _last(nb, scale, dk_in, dv_in, own_ref, got_ref, dk_hbm, dv_hbm, stage, sem):
    chip = lax.axis_index('cp') // 2
    hkv = own_ref.shape[2]
    outs = (dk_hbm, dv_hbm)

    def copies(n):
        return [pltpu.make_async_copy(stage.at[n, w], outs[w].at[nb - 2 * NL + n], sem.at[n, w]) for w in range(2)]

    def batch(n, terms):
        for sg in range(2):
            for w in range(2):
                x = [own_ref[n, sg, g, w] for g in range(hkv)]
                if terms[sg] is not None:
                    x = [y + got_ref[(*terms[sg], g, w)] for g, y in enumerate(x)]
                if w == 0:
                    x = [y * scale for y in x]
                stage[n, w, pl.ds(sg * C, C)] = jnp.stack(x, axis=1).astype(BF16)
        for copy in copies(n):
            copy.start()

    for c in range(2):
        @pl.when(chip == c)
        def _():
            for n in range(NL * c, 2 * NL):
                if n < NL:
                    batch(n, ((n, 1), None))
                else:
                    batch(n, ((n - NL, 0), (n - NL, 1) if c else None))
            for n in range(NL * c, 2 * NL):
                for copy in copies(n):
                    copy.wait()


def solution(mesh):
    swap = [(r, (r + 2) % 4) for r in range(4)]

    def local(q, k, v, do, o, lse):
        b, t, hq, d = q.shape
        hkv = k.shape[2]
        grp = hq // hkv
        scale = d ** -0.5
        ng = b // GB
        nr = len(range(R0, b - 2 * NL, RS))
        assert RLAG <= 2 * RS and LAG <= NO and LAG < 3 * RS and NL <= NP and 2 * NL <= NO
        heads = lambda x: jnp.transpose(x, (0, 2, 1, 3))
        q, do, o = (heads(x) for x in (q, do, o))
        lse = jnp.transpose(lse, (1, 0, 2))

        last = b - 1
        big = pl.BlockSpec((1, hq, t, d), lambda i: (jnp.minimum(i, last), 0, 0, 0))
        anyspec = pl.BlockSpec(memory_space=pl.ANY)
        dma = pltpu.SemaphoreType.DMA
        flops = 9 * b * hq * 5 * 2 * C * C * d
        shapes = [jax.ShapeDtypeStruct((b, hq, t, d), BF16),
                  jax.ShapeDtypeStruct((b, t, hkv, d), BF16),
                  jax.ShapeDtypeStruct((b, t, hkv, d), BF16)]
        dq, dk, dv, _, own, sums = pl.pallas_call(
            functools.partial(_kernel, b, hkv, grp, scale),
            grid=(b - NL + LAG,),
            in_specs=[big, big, big,
                      pl.BlockSpec((hq, 8, t), lambda i: (0, jnp.minimum(i, last) // 8, 0)),
                      anyspec, anyspec],
            out_specs=[big, *[anyspec] * 5],
            out_shape=[*shapes, *(jax.ShapeDtypeStruct((n, 2, hkv, 2, C, d), F32) for n in (b, 2 * NL, NL))],
            scratch_shapes=[
                pltpu.VMEM((b, 4, hkv, t, d), BF16),
                pltpu.VMEM((b, 4, hkv, t, d), BF16),
                pltpu.VMEM((2, GB, t, hkv, d), BF16),
                pltpu.VMEM((2, 8, hkv, 2, C, d), F32),
                pltpu.VMEM((2, 4, hkv, 2, C, d), F32),
                pltpu.VMEM((NP, 2, hkv, 2, C, d), F32),
                pltpu.VMEM((NO, 2, hkv, 2, C, d), F32),
                pltpu.VMEM((2, hkv, 2, C, d), F32),
                pltpu.VMEM((nr, 2, hkv, 2, C, d), F32),
                pltpu.VMEM((2, 2, hkv, 2, C, d), F32),
                pltpu.VMEM((2, t, hkv, d), BF16),
                pltpu.VMEM((2, t, hkv, d), BF16),
                pltpu.VMEM((2, hkv, d, grp * C), BF16),
                pltpu.VMEM((2, hkv, d, grp * C), BF16),
                pltpu.VMEM((2, hkv, d, grp * C), F32),
                pltpu.VMEM((2, hkv, 1, grp * C), F32),
                pltpu.VMEM((2, hkv, 1, grp * C), F32),
                dma((2,)), dma((ng, 2)), dma((ng, 2)), dma((ng, 2)), dma((ng, 2)), dma((ng, 2)), dma((ng, 2)),
                dma((2,)), dma((2,)), dma((NP,)), dma((b,)), dma(()),
                dma((2,)), dma((3,)), dma((nr,)), dma((2,)), dma((nr, 2)), dma((2 * NL, 2)), pltpu.SemaphoreType.REGULAR,
            ],
            compiler_params=pltpu.CompilerParams(
                dimension_semantics=('arbitrary',), collective_id=0, has_side_effects=True,
                vmem_limit_bytes=67043328),
            cost_estimate=pl.CostEstimate(flops=flops, bytes_accessed=4 * q.size * 2, transcendentals=0),
        )(q, do, o, lse, k, v)

        got = lax.ppermute(sums, 'cp', swap)
        two = [pl.BlockSpec((2, *x.shape[1:]), lambda i: (i, 0, 0, 0)) for x in shapes]
        dq, dk, dv = pl.pallas_call(
            _finish, grid=(b // 2,), in_specs=two, out_specs=two, out_shape=shapes,
            compiler_params=pltpu.CompilerParams(dimension_semantics=('arbitrary',)),
            cost_estimate=pl.CostEstimate(flops=10**8, bytes_accessed=4 * q.size, transcendentals=0),
        )(dq, dk, dv)
        one = pl.BlockSpec(memory_space=pltpu.VMEM)
        dk, dv = pl.pallas_call(
            functools.partial(_last, b, scale), in_specs=[anyspec, anyspec, one, one],
            out_specs=[anyspec, anyspec], out_shape=shapes[1:], input_output_aliases={0: 0, 1: 1},
            scratch_shapes=[pltpu.VMEM((2 * NL, 2, t, hkv, d), BF16), dma((2 * NL, 2))],
        )(dk, dv, own, got)
        return heads(dq), dk, dv

    spec = P('data', 'cp')
    return jax.shard_map(local, mesh=mesh, in_specs=(spec, spec, spec, spec, spec, P('data', None, 'cp')),
                         out_specs=(spec, spec, spec), check_vma=False)
```
